32 devices in a mesh: dp: 1 (over z), cx: 4 (over y), cy: 4 (over x), cz: 2 (over core).
Axes of the slice: x: 4, y: 4, z: 1, core: 2. Of those that a mesh axis runs over, the one named last changes fastest.
The devices are a block of a 4x4x8 slice.
Arguments:
- q: bfloat16 [2048, 64, 128], P(('dp', 'cx', 'cy', 'cz'))
- k: bfloat16 [2048, 8, 128], P(('dp', 'cx', 'cy', 'cz'))
- v: bfloat16 [2048, 8, 128], P(('dp', 'cx', 'cy', 'cz'))
Outputs:
- output: bfloat16 [2048, 64, 128], P(('dp', 'cx', 'cy', 'cz'))
All inputs are finite; a program needn't handle non-finite values.
Results may differ from the reference program's by a relative error of at most 0.00642288.
Values are sent between devices in bfloat16 or wider.
A program may use at most 768 MiB of HBM per device.

```python
import jax
import jax.numpy as jnp
from jax import lax

TOK = 64
DEV = 32
HQ = 64
HKV = 8
HEAD = 128


def setup_inputs(seed: int = 0, part: int = 0) -> dict:
    n = TOK * DEV
    key = jax.random.fold_in(jax.random.PRNGKey(seed), part)
    kq, kk, kv = jax.random.split(key, 3)
    q = jax.random.normal(kq, (n, HQ, HEAD), jnp.float32)
    k = jax.random.normal(kk, (n, HKV, HEAD), jnp.float32)
    v = jax.random.normal(kv, (n, HKV, HEAD), jnp.float32) * (0.5 * n ** 0.25)
    return {'q': q.astype(jnp.bfloat16), 'k': k.astype(jnp.bfloat16), 'v': v.astype(jnp.bfloat16)}


def reference(q, k, v):
    n = TOK * DEV
    g = HQ // HKV
    qb = min(n, 64)
    r = jnp.arange(n)
    pos = (r % TOK) * DEV + r // TOK
    kt = jnp.transpose(k, (1, 0, 2)).astype(jnp.float32)
    vt = jnp.transpose(v, (1, 0, 2)).astype(jnp.float32)
    qr = jnp.transpose(q.reshape(n // qb, qb, HKV, g, HEAD), (0, 2, 1, 3, 4))

    def head(qh, kh, vh, qp):
        s = jnp.einsum('qgd,kd->qgk', qh.astype(jnp.float32), kh) * HEAD ** -0.5
        s = jnp.where((pos[None, :] <= qp[:, None])[:, None, :], s, -jnp.inf)
        p = jnp.exp(s - jnp.max(s, axis=-1, keepdims=True))
        l = jnp.sum(p, axis=-1)
        o = jnp.einsum('qgk,kd->qgd', p.astype(jnp.bfloat16).astype(jnp.float32), vh)
        return o / l[..., None]

    def block(args):
        qblk, qp = args
        o = lax.map(lambda a: head(a[0], a[1], a[2], qp), (qblk, kt, vt))
        return jnp.transpose(o, (1, 0, 2, 3)).reshape(qb, HQ, HEAD)

    o = lax.map(block, (qr, pos.reshape(n // qb, qb)))
    return o.reshape(n, HQ, HEAD).astype(jnp.bfloat16)
```

```python
import functools
import math

import jax
import jax.numpy as jnp
from jax import lax
from jax.experimental import pallas as pl
from jax.experimental.pallas import tpu as pltpu
from jax.sharding import PartitionSpec as P

NEG = -1e30
RING = 4
LINKS = (("x", 1), ("x", -1), ("y", 1), ("y", -1))
HEAD_OF = {("x", 1): 0, ("x", -1): 1, ("y", 1): 2, ("y", -1): 3}
PLAN = (
    ("a", -1), ("b", -1), ("c", -1), ("d", -1), ("a", 0), ("c", 0), ("c", 1), ("d", 1),
    ("c", 4), ("c", 2), ("c", 5), ("c", 6), ("d", 0), ("c", 8), ("d", 4),
)
SLOTS = len(PLAN)
AHEAD = 4


def _head(link, letter):
    axis, sign = link
    other = "y" if axis == "x" else "x"
    return HEAD_OF[{"a": (axis, sign), "b": (axis, -sign), "c": (other, sign), "d": (other, -sign)}[letter]]


def _offsets():
    off = [dict() for _ in range(SLOTS)]
    for slot, (letter, src) in enumerate(PLAN):
        for link in LINKS:
            head = _head(link, letter)
            x, y = (0, 0) if src < 0 else off[src][head]
            axis, sign = link
            x, y = (x + sign, y) if axis == "x" else (x, y + sign)
            assert head not in off[slot]
            off[slot][head] = (x % RING, y % RING)
    for head in range(len(LINKS)):
        assert len({off[s][head] for s in range(SLOTS)} | {(0, 0)}) == RING * RING
    return off


OFF = _offsets()


def _kernel(k_hbm, v_hbm, q_hbm, o_hbm, kin, vin, st, kv, qs, qt, acc, m_ref, l_ref, ost, src,
            in_sem, x_sem, send_sem, recv_sem, out_sem):
    t, hkv, d = k_hbm.shape
    g = q_hbm.shape[2]
    hh = hkv // 2
    nb = t // 16
    w = 2 * 16 * g
    iy, ix, iz = lax.axis_index("cx"), lax.axis_index("cy"), lax.axis_index("cz")
    oz = 1 - iz
    chip = iy * RING + ix
    c = d ** -0.5 * math.log2(math.e)

    def peer(link):
        axis, sign = link
        if axis == "x":
            return {"cy": lax.rem(ix + sign + RING, RING)}
        return {"cx": lax.rem(iy + sign + RING, RING)}

    half = lambda z: pl.ds(pl.multiple_of(z * t, t), t)

    barrier = pltpu.get_barrier_semaphore()
    for link in LINKS:
        pl.semaphore_signal(barrier, inc=1, device_id=peer(link), device_id_type=pl.DeviceIdType.MESH)
    pl.semaphore_signal(barrier, inc=1, device_id={"cz": oz}, device_id_type=pl.DeviceIdType.MESH)
    k_in = pltpu.make_async_copy(k_hbm, kin, in_sem.at[0])
    v_in = pltpu.make_async_copy(v_hbm, vin, in_sem.at[1])
    q_in = pltpu.make_async_copy(q_hbm.at[:, pl.ds(hh * iz, hh)], qs.at[iz], in_sem.at[2])
    k_in.start()
    v_in.start()
    q_in.start()

    for n, (ref, copy) in enumerate(((kin, k_in), (vin, v_in))):
        copy.wait()
        x = jnp.swapaxes(ref[...].astype(jnp.float32), 0, 1)
        st[:, n] = x.astype(jnp.bfloat16)
    for h in range(hh):
        kv[0, h, :, half(iz), :] = st[hh * iz + h]

    def remote(a, b, s, r, to):
        return pltpu.make_async_remote_copy(
            src_ref=a, dst_ref=b, send_sem=s, recv_sem=r, device_id=to, device_id_type=pl.DeviceIdType.MESH)

    def unit(n, slot):
        link = LINKS[n]
        letter, arrival = PLAN[slot]
        h = _head(link, letter)
        sems = send_sem.at[n, slot], recv_sem.at[n, slot], peer(link)
        if slot < 2:
            return remote(st.at[hh * iz + h], kv.at[1 + slot, h, :, half(iz), :], *sems)
        return remote(kv.at[1 + arrival, h], kv.at[1 + slot, h], *sems)

    def rest(n, slot):
        link = LINKS[n]
        h = _head(link, PLAN[slot][0])
        return remote(kv.at[0, h, :, half(oz), :], kv.at[1 + slot, h, :, half(oz), :],
                      send_sem.at[n, SLOTS + slot], recv_sem.at[n, SLOTS + slot], peer(link))

    swap = remote(st.at[pl.ds(hh * oz, hh)], kv.at[0, :, :, half(iz), :], x_sem.at[0], x_sem.at[1], {"cz": oz})
    q_swap = remote(q_hbm.at[:, pl.ds(hh * oz, hh)], qs.at[iz], x_sem.at[2], x_sem.at[3], {"cz": oz})

    pl.semaphore_wait(barrier, len(LINKS) + 1)
    swap.start()
    for slot in range(2):
        for n in range(4):
            unit(n, slot).start()
    q_swap.start()
    swap.wait_recv()
    for slot in range(2):
        for n in range(4):
            rest(n, slot).start()
    for slot in range(2, AHEAD):
        for n in range(4):
            unit(n, slot).start()

    m_ref[...] = jnp.full_like(m_ref, NEG)
    l_ref[...] = jnp.zeros_like(l_ref)
    acc[...] = jnp.zeros_like(acc)

    def turn(p):
        @pl.loop(0, hh)
        def _(h):
            for a in range(nb):
                x = qs[p, 16 * a:16 * (a + 1), h].astype(jnp.float32).reshape(16 * g, d)
                qt[h, a, p] = x.T.astype(jnp.bfloat16)

    q_in.wait()
    q_swap.wait_recv()
    for p in range(2):
        turn(p)

    def step(k, carry):
        @pl.when(k == 0)
        def _():
            for h in range(hh):
                src[h] = chip

        for j in range(1, SLOTS + 1):
            @pl.when(k == j)
            def _():
                for n in range(4):
                    unit(n, j - 1).wait_recv()
                    if j - 1 < 2:
                        rest(n, j - 1).wait_recv()
                if j - 1 + AHEAD < SLOTS:
                    for n in range(4):
                        unit(n, j - 1 + AHEAD).start()
                for h in range(hh):
                    ox, oy = OFF[j - 1][h]
                    src[h] = lax.rem(iy - oy + RING, RING) * RING + lax.rem(ix - ox + RING, RING)

        lane = lax.broadcasted_iota(jnp.int32, (16, w), 1)
        row = lax.broadcasted_iota(jnp.int32, (16, w), 0)
        lead = lax.rem(lane, w // 2) // g - row
        for h in range(hh):
            vis = []
            for z in range(2):
                gap = 2 * (chip - src[h]) - z
                late = [jnp.where(gap + p >= 0, 0, 1) for p in range(2)]
                vis.append(lead >= jnp.where(lane < w // 2, late[0], late[1]))
            vt = kv[k, h, 1].T
            for a in range(nb):
                n = 16 * (a + 1)
                q = jnp.concatenate([qt[h, a, 0], qt[h, a, 1]], axis=1)
                s = []
                for z in range(2):
                    x = jnp.dot(kv[k, h, 0, z * t:z * t + n, :], q, preferred_element_type=jnp.float32)
                    edge = jnp.where(vis[z], x[n - 16:], NEG)
                    s.append(jnp.concatenate([x[:n - 16], edge], axis=0) if a else edge)
                old = m_ref[h, a]
                new = jnp.maximum(old, jnp.max(jnp.maximum(s[0], s[1]), axis=0, keepdims=True))
                m_ref[h, a] = new
                fade = jnp.exp2((old - new) * c)
                top = new * c
                e = [jnp.exp2(x * c - top) for x in s]
                l_ref[h, a] = l_ref[h, a] * fade + jnp.sum((e[0] + e[1]).reshape(n // 8, 8, w), axis=0)
                parts = []
                for x in e:
                    parts.append(x.astype(jnp.bfloat16))
                    if n < t:
                        parts.append(jnp.zeros((t - n, w), jnp.bfloat16))
                pv = jnp.dot(vt, jnp.concatenate(parts, axis=0), preferred_element_type=jnp.float32)
                acc[h, a] = acc[h, a] * fade + pv
        return carry

    lax.fori_loop(0, SLOTS + 1, step, 0)

    def out(h):
        mine = pltpu.make_async_copy(ost.at[iz, h], o_hbm.at[:, hh * iz + h], out_sem.at[0, h])
        theirs = remote(ost.at[oz, h], o_hbm.at[:, hh * iz + h], out_sem.at[1, h], out_sem.at[2, h], {"cz": oz})
        return mine, theirs

    @pl.loop(0, hh)
    def _(h):
        for a in range(nb):
            o = acc[h, a] * (1.0 / jnp.sum(l_ref[h, a], axis=0, keepdims=True))
            for p in range(2):
                x = o[:, p * 16 * g:(p + 1) * 16 * g].T
                ost[p, h, 16 * a:16 * (a + 1)] = x.reshape(16, g, d).astype(jnp.bfloat16)
        mine, theirs = out(h)
        theirs.start()
        mine.start()

    for slot in range(SLOTS):
        for n in range(4):
            unit(n, slot).wait_send()
            if slot < 2:
                rest(n, slot).wait_send()
    swap.wait_send()
    q_swap.wait_send()
    for h in range(hh):
        mine, theirs = out(h)
        mine.wait()
        theirs.wait_send()
        remote(ost.at[oz, h], o_hbm.at[:, hh * oz + h], out_sem.at[1, h], out_sem.at[2, h], {"cz": oz}).wait_recv()


def solution(mesh):
    assert mesh.shape["cx"] == RING and mesh.shape["cy"] == RING and mesh.shape["cz"] == 2
    spec = P(("dp", "cx", "cy", "cz"))

    def local(q, k, v):
        t, hq, d = q.shape
        hkv = k.shape[1]
        g = hq // hkv
        hh = hkv // 2
        nb = t // 16
        w = 2 * 16 * g
        units = SLOTS + 1
        o = pl.pallas_call(
            _kernel,
            out_shape=jax.ShapeDtypeStruct((t, hkv, g, d), jnp.bfloat16),
            in_specs=[pl.BlockSpec(memory_space=pl.ANY)] * 3,
            out_specs=pl.BlockSpec(memory_space=pl.ANY),
            scratch_shapes=[
                pltpu.VMEM((t, hkv, d), jnp.bfloat16),
                pltpu.VMEM((t, hkv, d), jnp.bfloat16),
                pltpu.VMEM((hkv, 2, t, d), jnp.bfloat16),
                pltpu.VMEM((units, hh, 2, 2 * t, d), jnp.bfloat16),
                pltpu.VMEM((2, t, hh, g, d), jnp.bfloat16),
                pltpu.VMEM((hh, nb, 2, d, 16 * g), jnp.bfloat16),
                pltpu.VMEM((hh, nb, d, w), jnp.float32),
                pltpu.VMEM((hh, nb, 1, w), jnp.float32),
                pltpu.VMEM((hh, nb, 8, w), jnp.float32),
                pltpu.VMEM((2, hh, t, g, d), jnp.bfloat16),
                pltpu.SMEM((hh,), jnp.int32),
                pltpu.SemaphoreType.DMA((3,)),
                pltpu.SemaphoreType.DMA((4,)),
                pltpu.SemaphoreType.DMA((4, SLOTS + 2)),
                pltpu.SemaphoreType.DMA((4, SLOTS + 2)),
                pltpu.SemaphoreType.DMA((3, hh)),
            ],
            compiler_params=pltpu.CompilerParams(collective_id=0, has_side_effects=True),
        )(k, v, q.reshape(t, hkv, g, d))
        return o.reshape(t, hq, d)

    return jax.shard_map(local, mesh=mesh, in_specs=(spec, spec, spec), out_specs=spec, check_vma=False)
```

```python
import functools
import math

import jax
import jax.numpy as jnp
from jax import lax
from jax.experimental import pallas as pl
from jax.experimental.pallas import tpu as pltpu
from jax.sharding import PartitionSpec as P

NEG = -1e30
RING = 4
LINKS = (("x", 1), ("x", -1), ("y", 1), ("y", -1))
HEAD_OF = {("x", 1): 0, ("x", -1): 1, ("y", 1): 2, ("y", -1): 3}
PLAN = (
    ("a", -1), ("b", -1), ("c", -1), ("d", -1), ("a", 0), ("c", 0), ("c", 1), ("d", 1),
    ("c", 4), ("c", 2), ("c", 5), ("c", 6), ("d", 0), ("c", 8), ("d", 4),
)
SLOTS = len(PLAN)
AHEAD = 4


def _head(link, letter):
    axis, sign = link
    other = "y" if axis == "x" else "x"
    return HEAD_OF[{"a": (axis, sign), "b": (axis, -sign), "c": (other, sign), "d": (other, -sign)}[letter]]


def _offsets():
    off = [dict() for _ in range(SLOTS)]
    for slot, (letter, src) in enumerate(PLAN):
        for link in LINKS:
            head = _head(link, letter)
            x, y = (0, 0) if src < 0 else off[src][head]
            axis, sign = link
            x, y = (x + sign, y) if axis == "x" else (x, y + sign)
            assert head not in off[slot]
            off[slot][head] = (x % RING, y % RING)
    for head in range(len(LINKS)):
        assert len({off[s][head] for s in range(SLOTS)} | {(0, 0)}) == RING * RING
    return off


OFF = _offsets()


def _kernel(k_hbm, v_hbm, q_hbm, o_ref, kin, vin, st, kv, qs, qt, acc, m_ref, l_ref, ost, src,
            in_sem, x_sem, send_sem, recv_sem, out_sem):
    t, hkv, d = k_hbm.shape
    g = q_hbm.shape[2]
    hh = hkv // 2
    nb = t // 16
    w = 2 * 16 * g
    iy, ix, iz = lax.axis_index("cx"), lax.axis_index("cy"), lax.axis_index("cz")
    oz = 1 - iz
    chip = iy * RING + ix
    c = d ** -0.5 * math.log2(math.e)

    def peer(link):
        axis, sign = link
        if axis == "x":
            return {"cy": lax.rem(ix + sign + RING, RING)}
        return {"cx": lax.rem(iy + sign + RING, RING)}

    half = lambda z: pl.ds(pl.multiple_of(z * t, t), t)

    k_in = pltpu.make_async_copy(k_hbm, kin, in_sem.at[0])
    v_in = pltpu.make_async_copy(v_hbm, vin, in_sem.at[1])
    q_in = pltpu.make_async_copy(q_hbm.at[:, pl.ds(hh * iz, hh)], qs.at[iz], in_sem.at[2])
    k_in.start()
    v_in.start()
    q_in.start()
    barrier = pltpu.get_barrier_semaphore()
    for link in LINKS:
        pl.semaphore_signal(barrier, inc=1, device_id=peer(link), device_id_type=pl.DeviceIdType.MESH)
    pl.semaphore_signal(barrier, inc=1, device_id={"cz": oz}, device_id_type=pl.DeviceIdType.MESH)

    for n, (ref, copy) in enumerate(((kin, k_in), (vin, v_in))):
        copy.wait()
        x = jnp.swapaxes(ref[...].astype(jnp.float32), 0, 1)
        st[:, n] = x.astype(jnp.bfloat16)
    for h in range(hh):
        kv[0, h, :, half(iz), :] = st[hh * iz + h]

    def remote(a, b, s, r, to):
        return pltpu.make_async_remote_copy(
            src_ref=a, dst_ref=b, send_sem=s, recv_sem=r, device_id=to, device_id_type=pl.DeviceIdType.MESH)

    def unit(n, slot):
        link = LINKS[n]
        letter, arrival = PLAN[slot]
        h = _head(link, letter)
        sems = send_sem.at[n, slot], recv_sem.at[n, slot], peer(link)
        if slot < 2:
            return remote(st.at[hh * iz + h], kv.at[1 + slot, h, :, half(iz), :], *sems)
        return remote(kv.at[1 + arrival, h], kv.at[1 + slot, h], *sems)

    def rest(n, slot):
        link = LINKS[n]
        h = _head(link, PLAN[slot][0])
        return remote(kv.at[0, h, :, half(oz), :], kv.at[1 + slot, h, :, half(oz), :],
                      send_sem.at[n, SLOTS + slot], recv_sem.at[n, SLOTS + slot], peer(link))

    swap = remote(st.at[pl.ds(hh * oz, hh)], kv.at[0, :, :, half(iz), :], x_sem.at[0], x_sem.at[1], {"cz": oz})
    q_swap = remote(q_hbm.at[:, pl.ds(hh * oz, hh)], qs.at[iz], x_sem.at[2], x_sem.at[3], {"cz": oz})

    pl.semaphore_wait(barrier, len(LINKS) + 1)
    swap.start()
    for slot in range(2):
        for n in range(4):
            unit(n, slot).start()
    q_swap.start()
    swap.wait_recv()
    for slot in range(2):
        for n in range(4):
            rest(n, slot).start()
    for slot in range(2, AHEAD):
        for n in range(4):
            unit(n, slot).start()

    m_ref[...] = jnp.full_like(m_ref, NEG)
    l_ref[...] = jnp.zeros_like(l_ref)
    acc[...] = jnp.zeros_like(acc)

    def turn(p):
        @pl.loop(0, hh)
        def _(h):
            for a in range(nb):
                x = qs[p, 16 * a:16 * (a + 1), h].astype(jnp.float32).reshape(16 * g, d)
                qt[h, a, p] = x.T.astype(jnp.bfloat16)

    q_in.wait()
    q_swap.wait_recv()
    for p in range(2):
        turn(p)

    def step(k, carry):
        @pl.when(k == 0)
        def _():
            for h in range(hh):
                src[h] = chip

        for j in range(1, SLOTS + 1):
            @pl.when(k == j)
            def _():
                for n in range(4):
                    unit(n, j - 1).wait_recv()
                    if j - 1 < 2:
                        rest(n, j - 1).wait_recv()
                for n in range(4):
                    if j >= 2:
                        unit(n, j - 2).wait_send()
                    if 2 <= j < 4:
                        rest(n, j - 2).wait_send()
                if j - 1 + AHEAD < SLOTS:
                    for n in range(4):
                        unit(n, j - 1 + AHEAD).start()
                for h in range(hh):
                    ox, oy = OFF[j - 1][h]
                    src[h] = lax.rem(iy - oy + RING, RING) * RING + lax.rem(ix - ox + RING, RING)

        lane = lax.broadcasted_iota(jnp.int32, (16, w), 1)
        row = lax.broadcasted_iota(jnp.int32, (16, w), 0)
        lead = lax.rem(lane, w // 2) // g - row
        for h in range(hh):
            vis = []
            for z in range(2):
                gap = 2 * (chip - src[h]) - z
                late = [jnp.where(gap + p >= 0, 0, 1) for p in range(2)]
                vis.append(lead >= jnp.where(lane < w // 2, late[0], late[1]))
            vt = kv[k, h, 1].T
            for a in range(nb):
                n = 16 * (a + 1)
                q = jnp.concatenate([qt[h, a, 0], qt[h, a, 1]], axis=1)
                s = []
                for z in range(2):
                    x = jnp.dot(kv[k, h, 0, z * t:z * t + n, :], q, preferred_element_type=jnp.float32)
                    edge = jnp.where(vis[z], x[n - 16:], NEG)
                    s.append(jnp.concatenate([x[:n - 16], edge], axis=0) if a else edge)
                old = m_ref[h, a]
                new = jnp.maximum(old, jnp.max(jnp.maximum(s[0], s[1]), axis=0, keepdims=True))
                m_ref[h, a] = new
                fade = jnp.exp2((old - new) * c)
                top = new * c
                e = [jnp.exp2(x * c - top) for x in s]
                l_ref[h, a] = l_ref[h, a] * fade + jnp.sum((e[0] + e[1]).reshape(n // 8, 8, w), axis=0)
                parts = []
                for x in e:
                    parts.append(x.astype(jnp.bfloat16))
                    if n < t:
                        parts.append(jnp.zeros((t - n, w), jnp.bfloat16))
                pv = jnp.dot(vt, jnp.concatenate(parts, axis=0), preferred_element_type=jnp.float32)
                acc[h, a] = acc[h, a] * fade + pv
        return carry

    swap.wait_send()
    q_swap.wait_send()
    lax.fori_loop(0, SLOTS + 1, step, 0)

    def out(h):
        return remote(ost.at[h], o_ref.at[:, hh * iz + h], out_sem.at[0, h], out_sem.at[1, h], {"cz": oz})

    @pl.loop(0, hh)
    def _(h):
        for a in range(nb):
            o = acc[h, a] * (1.0 / jnp.sum(l_ref[h, a], axis=0, keepdims=True))
            x = [o[:, p * 16 * g:(p + 1) * 16 * g].T.reshape(16, g, d).astype(jnp.bfloat16) for p in range(2)]
            here = iz == 0
            ost[h, 16 * a:16 * (a + 1)] = jnp.where(here, x[1], x[0])
            o_ref[16 * a:16 * (a + 1), hh * iz + h] = jnp.where(here, x[0], x[1])
        out(h).start()

    for n in range(4):
        unit(n, SLOTS - 1).wait_send()
    for h in range(hh):
        theirs = out(h)
        theirs.wait_send()
        theirs.wait_recv()


def solution(mesh):
    assert mesh.shape["cx"] == RING and mesh.shape["cy"] == RING and mesh.shape["cz"] == 2
    spec = P(("dp", "cx", "cy", "cz"))

    def local(q, k, v):
        t, hq, d = q.shape
        hkv = k.shape[1]
        g = hq // hkv
        hh = hkv // 2
        nb = t // 16
        w = 2 * 16 * g
        units = SLOTS + 1
        o = pl.pallas_call(
            _kernel,
            out_shape=jax.ShapeDtypeStruct((t, hkv, g, d), jnp.bfloat16),
            in_specs=[pl.BlockSpec(memory_space=pltpu.HBM)] * 3,
            out_specs=pl.BlockSpec(memory_space=pltpu.VMEM),
            scratch_shapes=[
                pltpu.VMEM((t, hkv, d), jnp.bfloat16),
                pltpu.VMEM((t, hkv, d), jnp.bfloat16),
                pltpu.VMEM((hkv, 2, t, d), jnp.bfloat16),
                pltpu.VMEM((units, hh, 2, 2 * t, d), jnp.bfloat16),
                pltpu.VMEM((2, t, hh, g, d), jnp.bfloat16),
                pltpu.VMEM((hh, nb, 2, d, 16 * g), jnp.bfloat16),
                pltpu.VMEM((hh, nb, d, w), jnp.float32),
                pltpu.VMEM((hh, nb, 1, w), jnp.float32),
                pltpu.VMEM((hh, nb, 8, w), jnp.float32),
                pltpu.VMEM((hh, t, g, d), jnp.bfloat16),
                pltpu.SMEM((hh,), jnp.int32),
                pltpu.SemaphoreType.DMA((3,)),
                pltpu.SemaphoreType.DMA((4,)),
                pltpu.SemaphoreType.DMA((4, SLOTS + 2)),
                pltpu.SemaphoreType.DMA((4, SLOTS + 2)),
                pltpu.SemaphoreType.DMA((2, hh)),
            ],
            compiler_params=pltpu.CompilerParams(collective_id=0, has_side_effects=True, vmem_limit_bytes=20 << 20),
        )(*(pltpu.with_memory_space_constraint(x, pltpu.HBM) for x in (k, v, q.reshape(t, hkv, g, d))))
        return o.reshape(t, hq, d)

    return jax.shard_map(local, mesh=mesh, in_specs=(spec, spec, spec), out_specs=spec, check_vma=False)
```

```python
import functools
import math

import jax
import jax.numpy as jnp
from jax import lax
from jax.experimental import pallas as pl
from jax.experimental.pallas import tpu as pltpu
from jax.sharding import PartitionSpec as P

NEG = -1e30
RING = 4
LINKS = (("x", 1), ("x", -1), ("y", 1), ("y", -1))
HEAD_OF = {("x", 1): 0, ("x", -1): 1, ("y", 1): 2, ("y", -1): 3}
PLAN = (
    ("a", -1), ("b", -1), ("c", -1), ("d", -1), ("a", 0), ("c", 0), ("c", 1), ("d", 1),
    ("c", 4), ("c", 2), ("c", 5), ("c", 6), ("d", 0), ("c", 8), ("d", 4),
)
SLOTS = len(PLAN)
AHEAD = 4
WHOLE = 11


def _head(link, letter):
    axis, sign = link
    other = "y" if axis == "x" else "x"
    return HEAD_OF[{"a": (axis, sign), "b": (axis, -sign), "c": (other, sign), "d": (other, -sign)}[letter]]


def _offsets():
    off = [dict() for _ in range(SLOTS)]
    for slot, (letter, src) in enumerate(PLAN):
        for link in LINKS:
            head = _head(link, letter)
            x, y = (0, 0) if src < 0 else off[src][head]
            axis, sign = link
            x, y = (x + sign, y) if axis == "x" else (x, y + sign)
            assert head not in off[slot]
            off[slot][head] = (x % RING, y % RING)
    for head in range(len(LINKS)):
        assert len({off[s][head] for s in range(SLOTS)} | {(0, 0)}) == RING * RING
    return off


OFF = _offsets()


def _kernel(k_hbm, v_hbm, q_hbm, o_ref, kin, vin, st, kv, qs, qt, acc, m_ref, l_ref, ost, sc, src,
            in_sem, x_sem, send_sem, recv_sem, out_sem):
    t, hkv, d = k_hbm.shape
    g = q_hbm.shape[2]
    hh = hkv // 2
    nb = t // 16
    w = 2 * 16 * g
    iy, ix, iz = lax.axis_index("cx"), lax.axis_index("cy"), lax.axis_index("cz")
    oz = 1 - iz
    chip = iy * RING + ix
    c = d ** -0.5 * math.log2(math.e)

    def peer(link):
        axis, sign = link
        if axis == "x":
            return {"cy": lax.rem(ix + sign + RING, RING)}
        return {"cx": lax.rem(iy + sign + RING, RING)}

    low, high = slice(0, t // 2), slice(t // 2, t)

    k_in = pltpu.make_async_copy(k_hbm, kin, in_sem.at[0])
    v_in = pltpu.make_async_copy(v_hbm, vin, in_sem.at[1])
    q_in = pltpu.make_async_copy(q_hbm.at[:, pl.ds(hh * iz, hh)], qs.at[iz], in_sem.at[2])
    k_in.start()
    v_in.start()
    q_in.start()
    barrier = pltpu.get_barrier_semaphore()
    for link in LINKS:
        pl.semaphore_signal(barrier, inc=1, device_id=peer(link), device_id_type=pl.DeviceIdType.MESH)
    pl.semaphore_signal(barrier, inc=1, device_id={"cz": oz}, device_id_type=pl.DeviceIdType.MESH)

    for n, (ref, copy) in enumerate(((kin, k_in), (vin, v_in))):
        copy.wait()
        x = jnp.swapaxes(ref[...].astype(jnp.float32), 0, 1)
        st[:, n] = x.astype(jnp.bfloat16)
    for h in range(hh):
        kv[0, h, :, iz] = st[hh * iz + h]

    def remote(a, b, s, r, to):
        return pltpu.make_async_remote_copy(
            src_ref=a, dst_ref=b, send_sem=s, recv_sem=r, device_id=to, device_id_type=pl.DeviceIdType.MESH)

    def unit(n, slot, part=0):
        link = LINKS[n]
        letter, arrival = PLAN[slot]
        h = _head(link, letter)
        here, there = kv.at[1 + arrival, h], kv.at[1 + slot, h]
        if slot < 2:
            z = (iz, oz)[part]
            here, there = (kv.at[0, h, :, z] if part else st.at[hh * iz + h]), there.at[:, z]
        elif slot >= WHOLE:
            rows = (low, high)[part]
            here, there = here.at[:, :, rows], there.at[:, :, rows]
        return remote(here, there, send_sem.at[part, n, slot], recv_sem.at[part, n, slot], peer(link))

    def parts(slot):
        return (0, 1) if slot < 2 or slot >= WHOLE else (0,)

    swap = remote(st.at[pl.ds(hh * oz, hh)], kv.at[0, :, :, iz], x_sem.at[0], x_sem.at[1], {"cz": oz})
    q_swap = remote(q_hbm.at[:, pl.ds(hh * oz, hh)], qs.at[iz], x_sem.at[2], x_sem.at[3], {"cz": oz})

    pl.semaphore_wait(barrier, len(LINKS) + 1)
    swap.start()
    for slot in range(2):
        for n in range(4):
            unit(n, slot).start()
    q_swap.start()
    swap.wait_recv()
    for slot in range(2):
        for n in range(4):
            unit(n, slot, 1).start()
    for slot in range(2, AHEAD):
        for n in range(4):
            unit(n, slot).start()

    m_ref[...] = jnp.full_like(m_ref, NEG)
    l_ref[...] = jnp.zeros_like(l_ref)
    acc[...] = jnp.zeros_like(acc)

    def turn(p):
        @pl.loop(0, hh)
        def _(h):
            for a in range(nb):
                x = qs[p, 16 * a:16 * (a + 1), h].astype(jnp.float32).reshape(16 * g, d)
                qt[h, a, p] = x.T.astype(jnp.bfloat16)

    q_in.wait()
    q_swap.wait_recv()
    for p in range(2):
        turn(p)

    def origin(slot):
        for h in range(hh):
            ox, oy = OFF[slot][h]
            src[slot + 1, h] = lax.rem(iy - oy + RING, RING) * RING + lax.rem(ix - ox + RING, RING)

    lane = lax.broadcasted_iota(jnp.int32, (16, w), 1)
    row = lax.broadcasted_iota(jnp.int32, (16, w), 0)
    lead = lax.rem(lane, w // 2) // g - row

    def attend(k, r0, r1):
        first = r0 // 16

        def scores(h, a):
            n = min(r1, 16 * (a + 1)) - r0
            q = jnp.concatenate([qt[h, a, 0], qt[h, a, 1]], axis=1)
            keys = jnp.concatenate([kv[k, h, 0, z, r0:r0 + n] for z in range(2)], axis=0)
            sc[h % 2, a, :2 * n] = jnp.dot(keys, q, preferred_element_type=jnp.float32)

        def weigh(h):
            vis = []
            for z in range(2):
                gap = 2 * (chip - src[k, h]) - z
                late = [jnp.where(gap + p >= 0, 0, 1) for p in range(2)]
                vis.append(lead >= jnp.where(lane < w // 2, late[0], late[1]))
            vt = kv[k, h, 1, :, r0:r1].reshape(2 * (r1 - r0), d).T
            for a in range(first, nb):
                n = min(r1, 16 * (a + 1)) - r0
                s = []
                for z in range(2):
                    x = sc[h % 2, a, z * n:(z + 1) * n]
                    if 16 * (a + 1) <= r1:
                        edge = jnp.where(vis[z], x[n - 16:], NEG)
                        x = jnp.concatenate([x[:n - 16], edge], axis=0) if n > 16 else edge
                    s.append(x)
                old = m_ref[h, a]
                new = jnp.maximum(old, jnp.max(jnp.maximum(s[0], s[1]), axis=0, keepdims=True))
                m_ref[h, a] = new
                fade = jnp.exp2((old - new) * c)
                top = new * c
                e = [jnp.exp2(x * c - top) for x in s]
                l_ref[h, a] = l_ref[h, a] * fade + jnp.sum((e[0] + e[1]).reshape(n // 8, 8, w), axis=0)
                weights = []
                for x in e:
                    weights.append(x.astype(jnp.bfloat16))
                    if n < r1 - r0:
                        weights.append(jnp.zeros((r1 - r0 - n, w), jnp.bfloat16))
                pv = jnp.dot(vt, jnp.concatenate(weights, axis=0), preferred_element_type=jnp.float32)
                acc[h, a] = acc[h, a] * fade + pv

        for a in range(first, nb):
            scores(0, a)
        for h in range(hh):
            if h + 1 < hh:
                for a in range(first, nb):
                    scores(h + 1, a)
            weigh(h)

    def finish(a0, a1):
        for h in range(hh):
            for a in range(a0, a1):
                o = acc[h, a] * (1.0 / jnp.sum(l_ref[h, a], axis=0, keepdims=True))
                x = [o[:, p * 16 * g:(p + 1) * 16 * g].T.reshape(16, g, d).astype(jnp.bfloat16) for p in range(2)]
                here = iz == 0
                ost[16 * a:16 * (a + 1), h] = jnp.where(here, x[1], x[0])
                o_ref[16 * a:16 * (a + 1), hh * iz + h] = jnp.where(here, x[0], x[1])

    def out(n):
        rows = (low, high)[n]
        return remote(ost.at[rows], o_ref.at[rows, pl.ds(hh * iz, hh)], out_sem.at[0, n], out_sem.at[1, n], {"cz": oz})

    tail = [(part, slot) for part in range(2) for slot in range(WHOLE, SLOTS)]
    first = WHOLE - AHEAD + 1
    late = {first: tail[:2], first + 1: tail[2:5], first + 2: tail[5:]}

    def whole(k, carry):
        for j in range(1, WHOLE + 1):
            @pl.when(k == j)
            def _():
                for n in range(4):
                    for part in parts(j - 1):
                        unit(n, j - 1, part).wait_recv()
                for n in range(4):
                    if j >= 2:
                        for part in parts(j - 2):
                            unit(n, j - 2, part).wait_send()
                if j - 1 + AHEAD < WHOLE:
                    for n in range(4):
                        unit(n, j - 1 + AHEAD).start()
                for part, slot in late.get(j, ()):
                    for n in range(4):
                        unit(n, slot, part).start()
        attend(k, 0, t)
        return carry

    def lows(k, carry):
        for n in range(4):
            land(n, k - 1, 0).wait_recv()
        attend(k, 0, t // 2)
        return carry

    def highs(k, carry):
        for n in range(4):
            land(n, k - 1, 1).wait_recv()
        attend(k, t // 2, t)
        return carry

    def land(n, slot, part):
        piece = kv.at[1 + slot, n].at[:, :, (low, high)[part]]
        return remote(piece, piece, send_sem.at[part, n, slot], recv_sem.at[part, n, slot], peer(LINKS[n]))

    for h in range(hh):
        src[0, h] = chip
    for slot in range(SLOTS):
        origin(slot)
    swap.wait_send()
    q_swap.wait_send()
    lax.fori_loop(0, WHOLE + 1, whole, 0)
    lax.fori_loop(WHOLE + 1, SLOTS + 1, lows, 0)
    finish(0, nb // 2)
    out(0).start()
    lax.fori_loop(WHOLE + 1, SLOTS + 1, highs, 0)
    finish(nb // 2, nb)
    out(1).start()
    for n in range(4):
        unit(n, WHOLE - 1).wait_send()
        for slot in range(WHOLE, SLOTS):
            for part in range(2):
                unit(n, slot, part).wait_send()
    for n in range(2):
        out(n).wait_send()
        out(n).wait_recv()


def solution(mesh):
    assert mesh.shape["cx"] == RING and mesh.shape["cy"] == RING and mesh.shape["cz"] == 2
    spec = P(("dp", "cx", "cy", "cz"))

    def local(q, k, v):
        t, hq, d = q.shape
        hkv = k.shape[1]
        g = hq // hkv
        hh = hkv // 2
        nb = t // 16
        w = 2 * 16 * g
        units = SLOTS + 1
        o = pl.pallas_call(
            _kernel,
            out_shape=jax.ShapeDtypeStruct((t, hkv, g, d), jnp.bfloat16),
            in_specs=[pl.BlockSpec(memory_space=pltpu.HBM)] * 3,
            out_specs=pl.BlockSpec(memory_space=pltpu.VMEM),
            scratch_shapes=[
                pltpu.VMEM((t, hkv, d), jnp.bfloat16),
                pltpu.VMEM((t, hkv, d), jnp.bfloat16),
                pltpu.VMEM((hkv, 2, t, d), jnp.bfloat16),
                pltpu.VMEM((units, hh, 2, 2, t, d), jnp.bfloat16),
                pltpu.VMEM((2, t, hh, g, d), jnp.bfloat16),
                pltpu.VMEM((hh, nb, 2, d, 16 * g), jnp.bfloat16),
                pltpu.VMEM((hh, nb, d, w), jnp.float32),
                pltpu.VMEM((hh, nb, 1, w), jnp.float32),
                pltpu.VMEM((hh, nb, 8, w), jnp.float32),
                pltpu.VMEM((t, hh, g, d), jnp.bfloat16),
                pltpu.VMEM((2, nb, 2 * t, w), jnp.float32),
                pltpu.SMEM((units, hh), jnp.int32),
                pltpu.SemaphoreType.DMA((3,)),
                pltpu.SemaphoreType.DMA((4,)),
                pltpu.SemaphoreType.DMA((2, 4, SLOTS)),
                pltpu.SemaphoreType.DMA((2, 4, SLOTS)),
                pltpu.SemaphoreType.DMA((2, 2)),
            ],
            compiler_params=pltpu.CompilerParams(collective_id=0, has_side_effects=True, vmem_limit_bytes=20 << 20),
        )(*(pltpu.with_memory_space_constraint(x, pltpu.HBM) for x in (k, v, q.reshape(t, hkv, g, d))))
        return o.reshape(t, hq, d)

    return jax.shard_map(local, mesh=mesh, in_specs=(spec, spec, spec), out_specs=spec, check_vma=False)
```

```python
import functools
import math

import jax
import jax.numpy as jnp
from jax import lax
from jax.experimental import pallas as pl
from jax.experimental.pallas import tpu as pltpu
from jax.sharding import PartitionSpec as P

NEG = -1e30
RING = 4
LINKS = (("x", 1), ("x", -1), ("y", 1), ("y", -1))
HEAD_OF = {("x", 1): 0, ("x", -1): 1, ("y", 1): 2, ("y", -1): 3}
PLAN = (
    ("a", -1), ("b", -1), ("c", -1), ("d", -1), ("a", 0), ("c", 0), ("c", 1), ("d", 1),
    ("c", 4), ("c", 2), ("c", 5), ("c", 6), ("d", 0), ("c", 8), ("d", 4),
)
SLOTS = len(PLAN)
AHEAD = 4


def _head(link, letter):
    axis, sign = link
    other = "y" if axis == "x" else "x"
    return HEAD_OF[{"a": (axis, sign), "b": (axis, -sign), "c": (other, sign), "d": (other, -sign)}[letter]]


def _offsets():
    off = [dict() for _ in range(SLOTS)]
    for slot, (letter, src) in enumerate(PLAN):
        for link in LINKS:
            head = _head(link, letter)
            x, y = (0, 0) if src < 0 else off[src][head]
            axis, sign = link
            x, y = (x + sign, y) if axis == "x" else (x, y + sign)
            assert head not in off[slot]
            off[slot][head] = (x % RING, y % RING)
    for head in range(len(LINKS)):
        assert len({off[s][head] for s in range(SLOTS)} | {(0, 0)}) == RING * RING
    return off


OFF = _offsets()


def _kernel(k_hbm, v_hbm, q_hbm, o_ref, kin, vin, st, kv, qs, qt, acc, m_ref, l_ref, ost, sc, src,
            in_sem, x_sem, send_sem, recv_sem, out_sem):
    t, hkv, d = k_hbm.shape
    g = q_hbm.shape[2]
    hh = hkv // 2
    nb = t // 16
    w = 2 * 16 * g
    iy, ix, iz = lax.axis_index("cx"), lax.axis_index("cy"), lax.axis_index("cz")
    oz = 1 - iz
    chip = iy * RING + ix
    c = d ** -0.5 * math.log2(math.e)

    def peer(link):
        axis, sign = link
        if axis == "x":
            return {"cy": lax.rem(ix + sign + RING, RING)}
        return {"cx": lax.rem(iy + sign + RING, RING)}

    half = lambda z: pl.ds(pl.multiple_of(z * t, t), t)

    k_in = pltpu.make_async_copy(k_hbm, kin, in_sem.at[0])
    v_in = pltpu.make_async_copy(v_hbm, vin, in_sem.at[1])
    q_in = pltpu.make_async_copy(q_hbm.at[:, pl.ds(hh * iz, hh)], qs.at[iz], in_sem.at[2])
    k_in.start()
    v_in.start()
    q_in.start()
    barrier = pltpu.get_barrier_semaphore()
    for link in LINKS:
        pl.semaphore_signal(barrier, inc=1, device_id=peer(link), device_id_type=pl.DeviceIdType.MESH)
    pl.semaphore_signal(barrier, inc=1, device_id={"cz": oz}, device_id_type=pl.DeviceIdType.MESH)

    for n, (ref, copy) in enumerate(((kin, k_in), (vin, v_in))):
        copy.wait()
        x = jnp.swapaxes(ref[...].astype(jnp.float32), 0, 1)
        st[:, n] = x.astype(jnp.bfloat16)
    for h in range(hh):
        kv[0, h, :, half(iz), :] = st[hh * iz + h]

    def remote(a, b, s, r, to):
        return pltpu.make_async_remote_copy(
            src_ref=a, dst_ref=b, send_sem=s, recv_sem=r, device_id=to, device_id_type=pl.DeviceIdType.MESH)

    def unit(n, slot):
        link = LINKS[n]
        letter, arrival = PLAN[slot]
        h = _head(link, letter)
        sems = send_sem.at[n, slot], recv_sem.at[n, slot], peer(link)
        if slot < 2:
            return remote(st.at[hh * iz + h], kv.at[1 + slot, h, :, half(iz), :], *sems)
        return remote(kv.at[1 + arrival, h], kv.at[1 + slot, h], *sems)

    def rest(n, slot):
        link = LINKS[n]
        h = _head(link, PLAN[slot][0])
        return remote(kv.at[0, h, :, half(oz), :], kv.at[1 + slot, h, :, half(oz), :],
                      send_sem.at[n, SLOTS + slot], recv_sem.at[n, SLOTS + slot], peer(link))

    swap = remote(st.at[pl.ds(hh * oz, hh)], kv.at[0, :, :, half(iz), :], x_sem.at[0], x_sem.at[1], {"cz": oz})
    q_swap = remote(q_hbm.at[:, pl.ds(hh * oz, hh)], qs.at[iz], x_sem.at[2], x_sem.at[3], {"cz": oz})

    pl.semaphore_wait(barrier, len(LINKS) + 1)
    swap.start()
    for slot in range(2):
        for n in range(4):
            unit(n, slot).start()
    q_swap.start()
    swap.wait_recv()
    for slot in range(2):
        for n in range(4):
            rest(n, slot).start()
    for slot in range(2, AHEAD):
        for n in range(4):
            unit(n, slot).start()

    m_ref[...] = jnp.full_like(m_ref, NEG)
    l_ref[...] = jnp.zeros_like(l_ref)
    acc[...] = jnp.zeros_like(acc)

    def turn(p):
        @pl.loop(0, hh)
        def _(h):
            for a in range(nb):
                x = qs[p, 16 * a:16 * (a + 1), h].astype(jnp.float32).reshape(16 * g, d)
                qt[h, a, p] = x.T.astype(jnp.bfloat16)

    q_in.wait()
    q_swap.wait_recv()
    for p in range(2):
        turn(p)

    def step(k, carry):
        @pl.when(k == 0)
        def _():
            for h in range(hh):
                src[h] = chip

        for j in range(1, SLOTS + 1):
            @pl.when(k == j)
            def _():
                for n in range(4):
                    unit(n, j - 1).wait_recv()
                    if j - 1 < 2:
                        rest(n, j - 1).wait_recv()
                for n in range(4):
                    if j >= 2:
                        unit(n, j - 2).wait_send()
                    if 2 <= j < 4:
                        rest(n, j - 2).wait_send()
                if j - 1 + AHEAD < SLOTS:
                    for n in range(4):
                        unit(n, j - 1 + AHEAD).start()
                for h in range(hh):
                    ox, oy = OFF[j - 1][h]
                    src[h] = lax.rem(iy - oy + RING, RING) * RING + lax.rem(ix - ox + RING, RING)

        lane = lax.broadcasted_iota(jnp.int32, (16, w), 1)
        row = lax.broadcasted_iota(jnp.int32, (16, w), 0)
        lead = lax.rem(lane, w // 2) // g - row
        def scores(h, a):
            n = 16 * (a + 1)
            q = jnp.concatenate([qt[h, a, 0], qt[h, a, 1]], axis=1)
            keys = jnp.concatenate([kv[k, h, 0, z * t:z * t + n, :] for z in range(2)], axis=0)
            sc[h % 2, a, :2 * n] = jnp.dot(keys, q, preferred_element_type=jnp.float32)

        def weigh(h):
            vis = []
            for z in range(2):
                gap = 2 * (chip - src[h]) - z
                late = [jnp.where(gap + p >= 0, 0, 1) for p in range(2)]
                vis.append(lead >= jnp.where(lane < w // 2, late[0], late[1]))
            vt = kv[k, h, 1].T
            for a in range(nb):
                n = 16 * (a + 1)
                s = []
                for z in range(2):
                    edge = jnp.where(vis[z], sc[h % 2, a, (z + 1) * n - 16:(z + 1) * n], NEG)
                    s.append(jnp.concatenate([sc[h % 2, a, z * n:(z + 1) * n - 16], edge], axis=0) if a else edge)
                old = m_ref[h, a]
                new = jnp.maximum(old, jnp.max(jnp.maximum(s[0], s[1]), axis=0, keepdims=True))
                m_ref[h, a] = new
                fade = jnp.exp2((old - new) * c)
                top = new * c
                e = [jnp.exp2(x * c - top) for x in s]
                l_ref[h, a] = l_ref[h, a] * fade + jnp.sum((e[0] + e[1]).reshape(n // 8, 8, w), axis=0)
                parts = []
                for x in e:
                    parts.append(x.astype(jnp.bfloat16))
                    if n < t:
                        parts.append(jnp.zeros((t - n, w), jnp.bfloat16))
                pv = jnp.dot(vt, jnp.concatenate(parts, axis=0), preferred_element_type=jnp.float32)
                acc[h, a] = acc[h, a] * fade + pv

        for a in range(nb):
            scores(0, a)
        for h in range(hh):
            if h + 1 < hh:
                for a in range(nb):
                    scores(h + 1, a)
            weigh(h)
        return carry

    swap.wait_send()
    q_swap.wait_send()
    lax.fori_loop(0, SLOTS + 1, step, 0)

    def out(h):
        return remote(ost.at[h], o_ref.at[:, hh * iz + h], out_sem.at[0, h], out_sem.at[1, h], {"cz": oz})

    @pl.loop(0, hh)
    def _(h):
        for a in range(nb):
            o = acc[h, a] * (1.0 / jnp.sum(l_ref[h, a], axis=0, keepdims=True))
            x = [o[:, p * 16 * g:(p + 1) * 16 * g].T.reshape(16, g, d).astype(jnp.bfloat16) for p in range(2)]
            here = iz == 0
            ost[h, 16 * a:16 * (a + 1)] = jnp.where(here, x[1], x[0])
            o_ref[16 * a:16 * (a + 1), hh * iz + h] = jnp.where(here, x[0], x[1])
        out(h).start()

    for n in range(4):
        unit(n, SLOTS - 1).wait_send()
    for h in range(hh):
        theirs = out(h)
        theirs.wait_send()
        theirs.wait_recv()


def solution(mesh):
    assert mesh.shape["cx"] == RING and mesh.shape["cy"] == RING and mesh.shape["cz"] == 2
    spec = P(("dp", "cx", "cy", "cz"))

    def local(q, k, v):
        t, hq, d = q.shape
        hkv = k.shape[1]
        g = hq // hkv
        hh = hkv // 2
        nb = t // 16
        w = 2 * 16 * g
        units = SLOTS + 1
        o = pl.pallas_call(
            _kernel,
            out_shape=jax.ShapeDtypeStruct((t, hkv, g, d), jnp.bfloat16),
            in_specs=[pl.BlockSpec(memory_space=pltpu.HBM)] * 3,
            out_specs=pl.BlockSpec(memory_space=pltpu.VMEM),
            scratch_shapes=[
                pltpu.VMEM((t, hkv, d), jnp.bfloat16),
                pltpu.VMEM((t, hkv, d), jnp.bfloat16),
                pltpu.VMEM((hkv, 2, t, d), jnp.bfloat16),
                pltpu.VMEM((units, hh, 2, 2 * t, d), jnp.bfloat16),
                pltpu.VMEM((2, t, hh, g, d), jnp.bfloat16),
                pltpu.VMEM((hh, nb, 2, d, 16 * g), jnp.bfloat16),
                pltpu.VMEM((hh, nb, d, w), jnp.float32),
                pltpu.VMEM((hh, nb, 1, w), jnp.float32),
                pltpu.VMEM((hh, nb, 8, w), jnp.float32),
                pltpu.VMEM((hh, t, g, d), jnp.bfloat16),
                pltpu.VMEM((2, nb, 2 * t, w), jnp.float32),
                pltpu.SMEM((hh,), jnp.int32),
                pltpu.SemaphoreType.DMA((3,)),
                pltpu.SemaphoreType.DMA((4,)),
                pltpu.SemaphoreType.DMA((4, SLOTS + 2)),
                pltpu.SemaphoreType.DMA((4, SLOTS + 2)),
                pltpu.SemaphoreType.DMA((2, hh)),
            ],
            compiler_params=pltpu.CompilerParams(collective_id=0, has_side_effects=True, vmem_limit_bytes=20 << 20),
        )(*(pltpu.with_memory_space_constraint(x, pltpu.HBM) for x in (k, v, q.reshape(t, hkv, g, d))))
        return o.reshape(t, hq, d)

    return jax.shard_map(local, mesh=mesh, in_specs=(spec, spec, spec), out_specs=spec, check_vma=False)
```

```python
import functools
import math

import jax
import jax.numpy as jnp
from jax import lax
from jax.experimental import pallas as pl
from jax.experimental.pallas import tpu as pltpu
from jax.sharding import PartitionSpec as P

NEG = -1e30
RING = 4
LINKS = (("x", 1), ("x", -1), ("y", 1), ("y", -1))
HEAD_OF = {("x", 1): 0, ("x", -1): 1, ("y", 1): 2, ("y", -1): 3}
PLAN = (
    ("a", -1), ("b", -1), ("c", -1), ("d", -1), ("a", 0), ("c", 0), ("c", 1), ("d", 1),
    ("c", 4), ("c", 2), ("c", 5), ("c", 6), ("d", 0), ("c", 8), ("d", 4),
)
SLOTS = len(PLAN)
AHEAD = 4


def _head(link, letter):
    axis, sign = link
    other = "y" if axis == "x" else "x"
    return HEAD_OF[{"a": (axis, sign), "b": (axis, -sign), "c": (other, sign), "d": (other, -sign)}[letter]]


def _offsets():
    off = [dict() for _ in range(SLOTS)]
    for slot, (letter, src) in enumerate(PLAN):
        for link in LINKS:
            head = _head(link, letter)
            x, y = (0, 0) if src < 0 else off[src][head]
            axis, sign = link
            x, y = (x + sign, y) if axis == "x" else (x, y + sign)
            assert head not in off[slot]
            off[slot][head] = (x % RING, y % RING)
    for head in range(len(LINKS)):
        assert len({off[s][head] for s in range(SLOTS)} | {(0, 0)}) == RING * RING
    return off


OFF = _offsets()


def _kernel(k_hbm, v_hbm, q_hbm, o_ref, kin, vin, st, kv, qs, qt, acc, m_ref, l_ref, ost, sc, src,
            in_sem, x_sem, send_sem, recv_sem, out_sem):
    t, hkv, d = k_hbm.shape
    g = q_hbm.shape[2]
    hh = hkv // 2
    nb = t // 16
    w = 2 * 16 * g
    iy, ix, iz = lax.axis_index("cx"), lax.axis_index("cy"), lax.axis_index("cz")
    oz = 1 - iz
    chip = iy * RING + ix
    c = d ** -0.5 * math.log2(math.e)

    def peer(link):
        axis, sign = link
        if axis == "x":
            return {"cy": lax.rem(ix + sign + RING, RING)}
        return {"cx": lax.rem(iy + sign + RING, RING)}

    half = lambda z: pl.ds(pl.multiple_of(z * t, t), t)

    k_in = pltpu.make_async_copy(k_hbm, kin, in_sem.at[0])
    v_in = pltpu.make_async_copy(v_hbm, vin, in_sem.at[1])
    q_in = pltpu.make_async_copy(q_hbm.at[:, pl.ds(hh * iz, hh)], qs.at[iz], in_sem.at[2])
    k_in.start()
    v_in.start()
    q_in.start()
    barrier = pltpu.get_barrier_semaphore()
    for link in LINKS:
        pl.semaphore_signal(barrier, inc=1, device_id=peer(link), device_id_type=pl.DeviceIdType.MESH)
    pl.semaphore_signal(barrier, inc=1, device_id={"cz": oz}, device_id_type=pl.DeviceIdType.MESH)

    for n, (ref, copy) in enumerate(((kin, k_in), (vin, v_in))):
        copy.wait()
        x = jnp.swapaxes(ref[...].astype(jnp.float32), 0, 1)
        st[:, n] = x.astype(jnp.bfloat16)
    for h in range(hh):
        kv[0, h, :, half(iz), :] = st[hh * iz + h]

    def remote(a, b, s, r, to):
        return pltpu.make_async_remote_copy(
            src_ref=a, dst_ref=b, send_sem=s, recv_sem=r, device_id=to, device_id_type=pl.DeviceIdType.MESH)

    def unit(n, slot):
        link = LINKS[n]
        letter, arrival = PLAN[slot]
        h = _head(link, letter)
        sems = send_sem.at[0], recv_sem.at[slot], peer(link)
        if slot < 2:
            return remote(st.at[hh * iz + h], kv.at[1 + slot, h, :, half(iz), :], *sems)
        return remote(kv.at[1 + arrival, h], kv.at[1 + slot, h], *sems)

    def landed(ref, sem):
        pltpu.make_async_copy(ref, ref, sem).wait()

    def rest(n, slot):
        link = LINKS[n]
        h = _head(link, PLAN[slot][0])
        return remote(kv.at[0, h, :, half(oz), :], kv.at[1 + slot, h, :, half(oz), :],
                      send_sem.at[0], recv_sem.at[slot], peer(link))

    swap = remote(st.at[pl.ds(hh * oz, hh)], kv.at[0, :, :, half(iz), :], x_sem.at[0], x_sem.at[1], {"cz": oz})
    q_swap = remote(q_hbm.at[:, pl.ds(hh * oz, hh)], qs.at[iz], x_sem.at[2], x_sem.at[3], {"cz": oz})

    pl.semaphore_wait(barrier, len(LINKS) + 1)
    swap.start()
    for slot in range(2):
        for n in range(4):
            unit(n, slot).start()
    q_swap.start()
    swap.wait_recv()
    for slot in range(2):
        for n in range(4):
            rest(n, slot).start()
    for slot in range(2, AHEAD):
        for n in range(4):
            unit(n, slot).start()

    m_ref[...] = jnp.full_like(m_ref, NEG)
    l_ref[...] = jnp.zeros_like(l_ref)
    acc[...] = jnp.zeros_like(acc)

    def turn(p):
        @pl.loop(0, hh)
        def _(h):
            for a in range(nb):
                x = qs[p, 16 * a:16 * (a + 1), h].astype(jnp.float32).reshape(16 * g, d)
                qt[h, a, p] = x.T.astype(jnp.bfloat16)

    q_in.wait()
    q_swap.wait_recv()
    for p in range(2):
        turn(p)

    def step(k, carry):
        @pl.when(k == 0)
        def _():
            for h in range(hh):
                src[h] = chip

        for j in range(1, SLOTS + 1):
            @pl.when(k == j)
            def _():
                landed(kv.at[j], recv_sem.at[j - 1])
                if j - 1 + AHEAD < SLOTS:
                    for n in range(4):
                        unit(n, j - 1 + AHEAD).start()
                for h in range(hh):
                    ox, oy = OFF[j - 1][h]
                    src[h] = lax.rem(iy - oy + RING, RING) * RING + lax.rem(ix - ox + RING, RING)

        lane = lax.broadcasted_iota(jnp.int32, (16, w), 1)
        row = lax.broadcasted_iota(jnp.int32, (16, w), 0)
        lead = lax.rem(lane, w // 2) // g - row
        def scores(h, a):
            n = 16 * (a + 1)
            q = jnp.concatenate([qt[h, a, 0], qt[h, a, 1]], axis=1)
            keys = jnp.concatenate([kv[k, h, 0, z * t:z * t + n, :] for z in range(2)], axis=0)
            sc[h % 2, a, :2 * n] = jnp.dot(keys, q, preferred_element_type=jnp.float32)

        def weigh(h):
            vis = []
            for z in range(2):
                gap = 2 * (chip - src[h]) - z
                late = [jnp.where(gap + p >= 0, 0, 1) for p in range(2)]
                vis.append(lead >= jnp.where(lane < w // 2, late[0], late[1]))
            vt = kv[k, h, 1].T
            for a in range(nb):
                n = 16 * (a + 1)
                s = []
                for z in range(2):
                    edge = jnp.where(vis[z], sc[h % 2, a, (z + 1) * n - 16:(z + 1) * n], NEG)
                    s.append(jnp.concatenate([sc[h % 2, a, z * n:(z + 1) * n - 16], edge], axis=0) if a else edge)
                old = m_ref[h, a]
                new = jnp.maximum(old, jnp.max(jnp.maximum(s[0], s[1]), axis=0, keepdims=True))
                m_ref[h, a] = new
                fade = jnp.exp2((old - new) * c)
                top = new * c
                e = [jnp.exp2(x * c - top) for x in s]
                l_ref[h, a] = l_ref[h, a] * fade + jnp.sum((e[0] + e[1]).reshape(n // 8, 8, w), axis=0)
                parts = []
                for x in e:
                    parts.append(x.astype(jnp.bfloat16))
                    if n < t:
                        parts.append(jnp.zeros((t - n, w), jnp.bfloat16))
                pv = jnp.dot(vt, jnp.concatenate(parts, axis=0), preferred_element_type=jnp.float32)
                acc[h, a] = acc[h, a] * fade + pv

        for a in range(nb):
            scores(0, a)
        for h in range(hh):
            if h + 1 < hh:
                for a in range(nb):
                    scores(h + 1, a)
            weigh(h)
        return carry

    swap.wait_send()
    q_swap.wait_send()
    lax.fori_loop(0, SLOTS + 1, step, 0)

    def out(h):
        return remote(ost.at[h], o_ref.at[:, hh * iz + h], out_sem.at[0], out_sem.at[1], {"cz": oz})

    @pl.loop(0, hh)
    def _(h):
        for a in range(nb):
            o = acc[h, a] * (1.0 / jnp.sum(l_ref[h, a], axis=0, keepdims=True))
            o = o.astype(jnp.bfloat16)
            x = [o[:, p * 16 * g:(p + 1) * 16 * g].T.reshape(16, g, d) for p in range(2)]
            here = iz == 0
            ost[h, 16 * a:16 * (a + 1)] = jnp.where(here, x[1], x[0])
            o_ref[16 * a:16 * (a + 1), hh * iz + h] = jnp.where(here, x[0], x[1])
        out(h).start()

    landed(kv.at[pl.ds(1, SLOTS)], send_sem.at[0])
    landed(ost, out_sem.at[0])
    landed(o_ref.at[:, pl.ds(hh * oz, hh)], out_sem.at[1])


def solution(mesh):
    assert mesh.shape["cx"] == RING and mesh.shape["cy"] == RING and mesh.shape["cz"] == 2
    spec = P(("dp", "cx", "cy", "cz"))

    def local(q, k, v):
        t, hq, d = q.shape
        hkv = k.shape[1]
        g = hq // hkv
        hh = hkv // 2
        nb = t // 16
        w = 2 * 16 * g
        units = SLOTS + 1
        o = pl.pallas_call(
            _kernel,
            out_shape=jax.ShapeDtypeStruct((t, hkv, g, d), jnp.bfloat16),
            in_specs=[pl.BlockSpec(memory_space=pltpu.HBM)] * 3,
            out_specs=pl.BlockSpec(memory_space=pltpu.VMEM),
            scratch_shapes=[
                pltpu.VMEM((t, hkv, d), jnp.bfloat16),
                pltpu.VMEM((t, hkv, d), jnp.bfloat16),
                pltpu.VMEM((hkv, 2, t, d), jnp.bfloat16),
                pltpu.VMEM((units, hh, 2, 2 * t, d), jnp.bfloat16),
                pltpu.VMEM((2, t, hh, g, d), jnp.bfloat16),
                pltpu.VMEM((hh, nb, 2, d, 16 * g), jnp.bfloat16),
                pltpu.VMEM((hh, nb, d, w), jnp.float32),
                pltpu.VMEM((hh, nb, 1, w), jnp.float32),
                pltpu.VMEM((hh, nb, 8, w), jnp.float32),
                pltpu.VMEM((hh, t, g, d), jnp.bfloat16),
                pltpu.VMEM((2, nb, 2 * t, w), jnp.float32),
                pltpu.SMEM((hh,), jnp.int32),
                pltpu.SemaphoreType.DMA((3,)),
                pltpu.SemaphoreType.DMA((4,)),
                pltpu.SemaphoreType.DMA((1,)),
                pltpu.SemaphoreType.DMA((SLOTS,)),
                pltpu.SemaphoreType.DMA((2,)),
            ],
            compiler_params=pltpu.CompilerParams(collective_id=0, has_side_effects=True, vmem_limit_bytes=20 << 20),
        )(*(pltpu.with_memory_space_constraint(x, pltpu.HBM) for x in (k, v, q.reshape(t, hkv, g, d))))
        return o.reshape(t, hq, d)

    return jax.shard_map(local, mesh=mesh, in_specs=(spec, spec, spec), out_specs=spec, check_vma=False)
```

```python
import functools
import math

import jax
import jax.numpy as jnp
from jax import lax
from jax.experimental import pallas as pl
from jax.experimental.pallas import tpu as pltpu
from jax.sharding import PartitionSpec as P

NEG = -1e30
RING = 4
LINKS = (("x", 1), ("x", -1), ("y", 1), ("y", -1))
HEAD_OF = {("x", 1): 0, ("x", -1): 1, ("y", 1): 2, ("y", -1): 3}
PLAN = (
    ("a", -1), ("b", -1), ("c", -1), ("d", -1), ("a", 0), ("c", 0), ("c", 1), ("d", 1),
    ("c", 4), ("c", 2), ("c", 5), ("c", 6), ("d", 0), ("c", 8), ("d", 4),
)
SLOTS = len(PLAN)
AHEAD = 4
LAG = 2


def _head(link, letter):
    axis, sign = link
    other = "y" if axis == "x" else "x"
    return HEAD_OF[{"a": (axis, sign), "b": (axis, -sign), "c": (other, sign), "d": (other, -sign)}[letter]]


def _offsets():
    off = [dict() for _ in range(SLOTS)]
    for slot, (letter, src) in enumerate(PLAN):
        for link in LINKS:
            head = _head(link, letter)
            x, y = (0, 0) if src < 0 else off[src][head]
            axis, sign = link
            x, y = (x + sign, y) if axis == "x" else (x, y + sign)
            assert head not in off[slot]
            off[slot][head] = (x % RING, y % RING)
    for head in range(len(LINKS)):
        assert len({off[s][head] for s in range(SLOTS)} | {(0, 0)}) == RING * RING
    return off


OFF = _offsets()


def _kernel(k_hbm, v_hbm, q_hbm, o_ref, kin, vin, st, kv, qs, qt, acc, m_ref, l_ref, ost, sc, src,
            in_sem, x_sem, send_sem, recv_sem, out_sem):
    t, hkv, d = k_hbm.shape
    g = q_hbm.shape[2]
    hh = hkv // 2
    nb = t // 16
    w = 2 * 16 * g
    iy, ix, iz = lax.axis_index("cx"), lax.axis_index("cy"), lax.axis_index("cz")
    oz = 1 - iz
    chip = iy * RING + ix
    c = d ** -0.5 * math.log2(math.e)

    def peer(link):
        axis, sign = link
        if axis == "x":
            return {"cy": lax.rem(ix + sign + RING, RING)}
        return {"cx": lax.rem(iy + sign + RING, RING)}

    half = lambda z: pl.ds(pl.multiple_of(z * t, t), t)

    k_in = pltpu.make_async_copy(k_hbm, kin, in_sem.at[0])
    v_in = pltpu.make_async_copy(v_hbm, vin, in_sem.at[1])
    q_in = pltpu.make_async_copy(q_hbm.at[:, pl.ds(hh * iz, hh)], qs.at[iz], in_sem.at[2])
    k_in.start()
    v_in.start()
    q_in.start()
    barrier = pltpu.get_barrier_semaphore()
    for link in LINKS:
        pl.semaphore_signal(barrier, inc=1, device_id=peer(link), device_id_type=pl.DeviceIdType.MESH)
    pl.semaphore_signal(barrier, inc=1, device_id={"cz": oz}, device_id_type=pl.DeviceIdType.MESH)

    for n, (ref, copy) in enumerate(((kin, k_in), (vin, v_in))):
        copy.wait()
        x = jnp.swapaxes(ref[...].astype(jnp.float32), 0, 1)
        st[:, n] = x.astype(jnp.bfloat16)
    for h in range(hh):
        kv[0, h, :, half(iz), :] = st[hh * iz + h]

    def remote(a, b, s, r, to):
        return pltpu.make_async_remote_copy(
            src_ref=a, dst_ref=b, send_sem=s, recv_sem=r, device_id=to, device_id_type=pl.DeviceIdType.MESH)

    def unit(n, slot):
        link = LINKS[n]
        letter, arrival = PLAN[slot]
        h = _head(link, letter)
        sems = send_sem.at[0], recv_sem.at[slot], peer(link)
        if slot < 2:
            return remote(st.at[hh * iz + h], kv.at[1 + slot, h, :, half(iz), :], *sems)
        return remote(kv.at[1 + arrival, h], kv.at[1 + slot, h], *sems)

    def landed(ref, sem):
        pltpu.make_async_copy(ref, ref, sem).wait()

    def rest(n, slot):
        link = LINKS[n]
        h = _head(link, PLAN[slot][0])
        return remote(kv.at[0, h, :, half(oz), :], kv.at[1 + slot, h, :, half(oz), :],
                      send_sem.at[0], recv_sem.at[slot], peer(link))

    swap = remote(st.at[pl.ds(hh * oz, hh)], kv.at[0, :, :, half(iz), :], x_sem.at[0], x_sem.at[1], {"cz": oz})
    q_swap = remote(q_hbm.at[:, pl.ds(hh * oz, hh)], qs.at[iz], x_sem.at[2], x_sem.at[3], {"cz": oz})

    pl.semaphore_wait(barrier, len(LINKS) + 1)
    swap.start()
    for slot in range(2):
        for n in range(4):
            unit(n, slot).start()
    q_swap.start()
    swap.wait_recv()
    for slot in range(2):
        for n in range(4):
            rest(n, slot).start()
    for slot in range(2, AHEAD):
        for n in range(4):
            unit(n, slot).start()

    m_ref[...] = jnp.full_like(m_ref, NEG)
    l_ref[...] = jnp.zeros_like(l_ref)
    acc[...] = jnp.zeros_like(acc)

    def turn(p):
        @pl.loop(0, hh)
        def _(h):
            for a in range(nb):
                x = qs[p, 16 * a:16 * (a + 1), h].astype(jnp.float32).reshape(16 * g, d)
                qt[h, a, p] = x.T.astype(jnp.bfloat16)

    q_in.wait()
    q_swap.wait_recv()
    for p in range(2):
        turn(p)

    def step(k, carry):
        @pl.when(k == 0)
        def _():
            for h in range(hh):
                src[h] = chip

        for j in range(1, SLOTS + 1):
            @pl.when(k == j)
            def _():
                landed(kv.at[j], recv_sem.at[j - 1])
                if j - 1 + AHEAD < SLOTS - 1:
                    for n in range(4):
                        unit(n, j - 1 + AHEAD).start()
                if j - 1 + AHEAD == SLOTS - 1:
                    @pl.when(iz == 0)
                    def _():
                        for n in range(4):
                            unit(n, SLOTS - 1).start()
                if j == SLOTS - LAG:
                    @pl.when(iz == 1)
                    def _():
                        for n in range(4):
                            unit(n, SLOTS - 1).start()
                for h in range(hh):
                    ox, oy = OFF[j - 1][h]
                    src[h] = lax.rem(iy - oy + RING, RING) * RING + lax.rem(ix - ox + RING, RING)

        lane = lax.broadcasted_iota(jnp.int32, (16, w), 1)
        row = lax.broadcasted_iota(jnp.int32, (16, w), 0)
        lead = lax.rem(lane, w // 2) // g - row
        def scores(h, a):
            n = 16 * (a + 1)
            q = jnp.concatenate([qt[h, a, 0], qt[h, a, 1]], axis=1)
            keys = jnp.concatenate([kv[k, h, 0, z * t:z * t + n, :] for z in range(2)], axis=0)
            sc[h % 2, a, :2 * n] = jnp.dot(keys, q, preferred_element_type=jnp.float32)

        def weigh(h):
            vis = []
            for z in range(2):
                gap = 2 * (chip - src[h]) - z
                late = [jnp.where(gap + p >= 0, 0, 1) for p in range(2)]
                vis.append(lead >= jnp.where(lane < w // 2, late[0], late[1]))
            vt = kv[k, h, 1].T
            for a in range(nb):
                n = 16 * (a + 1)
                s = []
                for z in range(2):
                    edge = jnp.where(vis[z], sc[h % 2, a, (z + 1) * n - 16:(z + 1) * n], NEG)
                    s.append(jnp.concatenate([sc[h % 2, a, z * n:(z + 1) * n - 16], edge], axis=0) if a else edge)
                old = m_ref[h, a]
                new = jnp.maximum(old, jnp.max(jnp.maximum(s[0], s[1]), axis=0, keepdims=True))
                m_ref[h, a] = new
                fade = jnp.exp2((old - new) * c)
                top = new * c
                e = [jnp.exp2(x * c - top) for x in s]
                l_ref[h, a] = l_ref[h, a] * fade + jnp.sum((e[0] + e[1]).reshape(n // 8, 8, w), axis=0)
                parts = []
                for x in e:
                    parts.append(x.astype(jnp.bfloat16))
                    if n < t:
                        parts.append(jnp.zeros((t - n, w), jnp.bfloat16))
                pv = jnp.dot(vt, jnp.concatenate(parts, axis=0), preferred_element_type=jnp.float32)
                acc[h, a] = acc[h, a] * fade + pv

        for a in range(nb):
            scores(0, a)
        for h in range(hh):
            if h + 1 < hh:
                for a in range(nb):
                    scores(h + 1, a)
            weigh(h)
        return carry

    swap.wait_send()
    q_swap.wait_send()
    lax.fori_loop(0, SLOTS + 1, step, 0)

    def out(h):
        return remote(ost.at[h], o_ref.at[:, hh * iz + h], out_sem.at[0], out_sem.at[1], {"cz": oz})

    @pl.loop(0, hh)
    def _(h):
        for a in range(nb):
            o = acc[h, a] * (1.0 / jnp.sum(l_ref[h, a], axis=0, keepdims=True))
            o = o.astype(jnp.bfloat16)
            x = [o[:, p * 16 * g:(p + 1) * 16 * g].T.reshape(16, g, d) for p in range(2)]
            here = iz == 0
            ost[h, 16 * a:16 * (a + 1)] = jnp.where(here, x[1], x[0])
            o_ref[16 * a:16 * (a + 1), hh * iz + h] = jnp.where(here, x[0], x[1])
        out(h).start()

    landed(kv.at[pl.ds(1, SLOTS)], send_sem.at[0])
    landed(ost, out_sem.at[0])
    landed(o_ref.at[:, pl.ds(hh * oz, hh)], out_sem.at[1])


def solution(mesh):
    assert mesh.shape["cx"] == RING and mesh.shape["cy"] == RING and mesh.shape["cz"] == 2
    spec = P(("dp", "cx", "cy", "cz"))

    def local(q, k, v):
        t, hq, d = q.shape
        hkv = k.shape[1]
        g = hq // hkv
        hh = hkv // 2
        nb = t // 16
        w = 2 * 16 * g
        units = SLOTS + 1
        o = pl.pallas_call(
            _kernel,
            out_shape=jax.ShapeDtypeStruct((t, hkv, g, d), jnp.bfloat16),
            in_specs=[pl.BlockSpec(memory_space=pltpu.HBM)] * 3,
            out_specs=pl.BlockSpec(memory_space=pltpu.VMEM),
            scratch_shapes=[
                pltpu.VMEM((t, hkv, d), jnp.bfloat16),
                pltpu.VMEM((t, hkv, d), jnp.bfloat16),
                pltpu.VMEM((hkv, 2, t, d), jnp.bfloat16),
                pltpu.VMEM((units, hh, 2, 2 * t, d), jnp.bfloat16),
                pltpu.VMEM((2, t, hh, g, d), jnp.bfloat16),
                pltpu.VMEM((hh, nb, 2, d, 16 * g), jnp.bfloat16),
                pltpu.VMEM((hh, nb, d, w), jnp.float32),
                pltpu.VMEM((hh, nb, 1, w), jnp.float32),
                pltpu.VMEM((hh, nb, 8, w), jnp.float32),
                pltpu.VMEM((hh, t, g, d), jnp.bfloat16),
                pltpu.VMEM((2, nb, 2 * t, w), jnp.float32),
                pltpu.SMEM((hh,), jnp.int32),
                pltpu.SemaphoreType.DMA((3,)),
                pltpu.SemaphoreType.DMA((4,)),
                pltpu.SemaphoreType.DMA((1,)),
                pltpu.SemaphoreType.DMA((SLOTS,)),
                pltpu.SemaphoreType.DMA((2,)),
            ],
            compiler_params=pltpu.CompilerParams(collective_id=0, has_side_effects=True, vmem_limit_bytes=20 << 20),
        )(*(pltpu.with_memory_space_constraint(x, pltpu.HBM) for x in (k, v, q.reshape(t, hkv, g, d))))
        return o.reshape(t, hq, d)

    return jax.shard_map(local, mesh=mesh, in_specs=(spec, spec, spec), out_specs=spec, check_vma=False)
```

```python
import functools
import math

import jax
import jax.numpy as jnp
from jax import lax
from jax.experimental import pallas as pl
from jax.experimental.pallas import tpu as pltpu
from jax.sharding import PartitionSpec as P

NEG = -1e30
RING = 4
LINKS = (("x", 1), ("x", -1), ("y", 1), ("y", -1))
HEAD_OF = {("x", 1): 0, ("x", -1): 1, ("y", 1): 2, ("y", -1): 3}
PLAN = (
    ("a", -1), ("b", -1), ("c", -1), ("d", -1), ("a", 0), ("c", 0), ("c", 1), ("d", 1),
    ("c", 4), ("c", 2), ("c", 5), ("c", 6), ("d", 0), ("c", 8), ("d", 4),
)
SLOTS = len(PLAN)
AHEAD = 4
WHOLE = SLOTS - 2
LAG = 2


def _head(link, letter):
    axis, sign = link
    other = "y" if axis == "x" else "x"
    return HEAD_OF[{"a": (axis, sign), "b": (axis, -sign), "c": (other, sign), "d": (other, -sign)}[letter]]


def _offsets():
    off = [dict() for _ in range(SLOTS)]
    for slot, (letter, src) in enumerate(PLAN):
        for link in LINKS:
            head = _head(link, letter)
            x, y = (0, 0) if src < 0 else off[src][head]
            axis, sign = link
            x, y = (x + sign, y) if axis == "x" else (x, y + sign)
            assert head not in off[slot]
            off[slot][head] = (x % RING, y % RING)
    for head in range(len(LINKS)):
        assert len({off[s][head] for s in range(SLOTS)} | {(0, 0)}) == RING * RING
    return off


OFF = _offsets()


def _kernel(k_hbm, v_hbm, q_hbm, o_ref, kin, vin, st, kv, qs, qt, acc, m_ref, l_ref, ost, sc, src,
            in_sem, x_sem, send_sem, recv_sem, out_sem):
    t, hkv, d = k_hbm.shape
    g = q_hbm.shape[2]
    hh = hkv // 2
    nb = t // 16
    w = 2 * 16 * g
    iy, ix, iz = lax.axis_index("cx"), lax.axis_index("cy"), lax.axis_index("cz")
    oz = 1 - iz
    chip = iy * RING + ix
    c = d ** -0.5 * math.log2(math.e)

    def peer(link):
        axis, sign = link
        if axis == "x":
            return {"cy": lax.rem(ix + sign + RING, RING)}
        return {"cx": lax.rem(iy + sign + RING, RING)}

    low, high = slice(0, t // 2), slice(t // 2, t)

    k_in = pltpu.make_async_copy(k_hbm, kin, in_sem.at[0])
    v_in = pltpu.make_async_copy(v_hbm, vin, in_sem.at[1])
    q_in = pltpu.make_async_copy(q_hbm.at[:, pl.ds(hh * iz, hh)], qs.at[iz], in_sem.at[2])
    k_in.start()
    v_in.start()
    q_in.start()
    barrier = pltpu.get_barrier_semaphore()
    for link in LINKS:
        pl.semaphore_signal(barrier, inc=1, device_id=peer(link), device_id_type=pl.DeviceIdType.MESH)
    pl.semaphore_signal(barrier, inc=1, device_id={"cz": oz}, device_id_type=pl.DeviceIdType.MESH)

    for n, (ref, copy) in enumerate(((kin, k_in), (vin, v_in))):
        copy.wait()
        x = jnp.swapaxes(ref[...].astype(jnp.float32), 0, 1)
        st[:, n] = x.astype(jnp.bfloat16)
    for h in range(hh):
        kv[0, h, :, iz] = st[hh * iz + h]

    def remote(a, b, s, r, to):
        return pltpu.make_async_remote_copy(
            src_ref=a, dst_ref=b, send_sem=s, recv_sem=r, device_id=to, device_id_type=pl.DeviceIdType.MESH)

    def unit(n, slot, part=0):
        link = LINKS[n]
        letter, arrival = PLAN[slot]
        h = _head(link, letter)
        here, there, to = kv.at[1 + arrival, h], kv.at[1 + slot, h], slot
        if slot < 2:
            z = (iz, oz)[part]
            here, there = (kv.at[0, h, :, z] if part else st.at[hh * iz + h]), there.at[:, z]
        elif slot >= WHOLE:
            rows, to = (low, high)[part], WHOLE + part
            here, there = here.at[:, :, rows], there.at[:, :, rows]
        return remote(here, there, send_sem.at[0], recv_sem.at[to], peer(link))

    def landed(ref, sem):
        pltpu.make_async_copy(ref, ref, sem).wait()

    swap = remote(st.at[pl.ds(hh * oz, hh)], kv.at[0, :, :, iz], x_sem.at[0], x_sem.at[1], {"cz": oz})
    q_swap = remote(q_hbm.at[:, pl.ds(hh * oz, hh)], qs.at[iz], x_sem.at[2], x_sem.at[3], {"cz": oz})

    pl.semaphore_wait(barrier, len(LINKS) + 1)
    swap.start()
    for slot in range(2):
        for n in range(4):
            unit(n, slot).start()
    q_swap.start()
    swap.wait_recv()
    for slot in range(2):
        for n in range(4):
            unit(n, slot, 1).start()
    for slot in range(2, AHEAD):
        for n in range(4):
            unit(n, slot).start()

    m_ref[...] = jnp.full_like(m_ref, NEG)
    l_ref[...] = jnp.zeros_like(l_ref)
    acc[...] = jnp.zeros_like(acc)

    def turn(p):
        @pl.loop(0, hh)
        def _(h):
            for a in range(nb):
                x = qs[p, 16 * a:16 * (a + 1), h].astype(jnp.float32).reshape(16 * g, d)
                qt[h, a, p] = x.T.astype(jnp.bfloat16)

    q_in.wait()
    q_swap.wait_recv()
    for p in range(2):
        turn(p)

    def origin(slot):
        for h in range(hh):
            ox, oy = OFF[slot][h]
            src[slot + 1, h] = lax.rem(iy - oy + RING, RING) * RING + lax.rem(ix - ox + RING, RING)

    lane = lax.broadcasted_iota(jnp.int32, (16, w), 1)
    row = lax.broadcasted_iota(jnp.int32, (16, w), 0)
    lead = lax.rem(lane, w // 2) // g - row

    def attend(units, r0, r1):
        first = r0 // 16
        pieces = [(k, z) for k in units for z in range(2)]

        def scores(h, a):
            n = min(r1, 16 * (a + 1)) - r0
            q = jnp.concatenate([qt[h, a, 0], qt[h, a, 1]], axis=1)
            keys = jnp.concatenate([kv[k, h, 0, z, r0:r0 + n] for k, z in pieces], axis=0)
            sc[h % 2, a, :len(pieces) * n] = jnp.dot(keys, q, preferred_element_type=jnp.float32)

        def weigh(h):
            vis = []
            for k, z in pieces:
                gap = 2 * (chip - src[k, h]) - z
                late = [jnp.where(gap + p >= 0, 0, 1) for p in range(2)]
                vis.append(lead >= jnp.where(lane < w // 2, late[0], late[1]))
            vt = jnp.concatenate([kv[k, h, 1, z, r0:r1] for k, z in pieces], axis=0).T
            for a in range(first, nb):
                n = min(r1, 16 * (a + 1)) - r0
                s = []
                for i in range(len(pieces)):
                    x = sc[h % 2, a, i * n:(i + 1) * n]
                    if 16 * (a + 1) <= r1:
                        edge = jnp.where(vis[i], x[n - 16:], NEG)
                        x = jnp.concatenate([x[:n - 16], edge], axis=0) if n > 16 else edge
                    s.append(x)
                old = m_ref[h, a]
                new = jnp.maximum(old, jnp.max(functools.reduce(jnp.maximum, s), axis=0, keepdims=True))
                m_ref[h, a] = new
                fade = jnp.exp2((old - new) * c)
                top = new * c
                e = [jnp.exp2(x * c - top) for x in s]
                l_ref[h, a] = l_ref[h, a] * fade + jnp.sum(sum(e[1:], e[0]).reshape(n // 8, 8, w), axis=0)
                weights = []
                for x in e:
                    weights.append(x.astype(jnp.bfloat16))
                    if n < r1 - r0:
                        weights.append(jnp.zeros((r1 - r0 - n, w), jnp.bfloat16))
                pv = jnp.dot(vt, jnp.concatenate(weights, axis=0), preferred_element_type=jnp.float32)
                acc[h, a] = acc[h, a] * fade + pv

        for a in range(first, nb):
            scores(0, a)
        for h in range(hh):
            if h + 1 < hh:
                for a in range(first, nb):
                    scores(h + 1, a)
            weigh(h)

    def out(h, rows):
        return remote(ost.at[h, rows], o_ref.at[rows, hh * iz + h], out_sem.at[0], out_sem.at[1], {"cz": oz})

    def finish(a0, a1):
        @pl.loop(0, hh)
        def _(h):
            for a in range(a0, a1):
                o = (acc[h, a] * (1.0 / jnp.sum(l_ref[h, a], axis=0, keepdims=True))).astype(jnp.bfloat16)
                x = [o[:, p * 16 * g:(p + 1) * 16 * g].T.reshape(16, g, d) for p in range(2)]
                here = iz == 0
                ost[h, 16 * a:16 * (a + 1)] = jnp.where(here, x[1], x[0])
                o_ref[16 * a:16 * (a + 1), hh * iz + h] = jnp.where(here, x[0], x[1])
            out(h, slice(16 * a0, 16 * a1)).start()

    def send_last(part):
        for slot in range(WHOLE, SLOTS):
            for n in range(4):
                unit(n, slot, part).start()

    def step(k, carry):
        for j in range(1, WHOLE + 1):
            @pl.when(k == j)
            def _():
                landed(kv.at[j], recv_sem.at[j - 1])
                if j - 1 + AHEAD < WHOLE:
                    for n in range(4):
                        unit(n, j - 1 + AHEAD).start()
                if j - 1 + AHEAD == WHOLE:
                    send_last(0)
                if j - 1 + AHEAD == WHOLE + 1:
                    @pl.when(iz == 0)
                    def _():
                        send_last(1)
                if j == SLOTS - LAG:
                    @pl.when(iz == 1)
                    def _():
                        send_last(1)
        attend((k,), 0, t)
        return carry

    for h in range(hh):
        src[0, h] = chip
    for slot in range(SLOTS):
        origin(slot)
    swap.wait_send()
    q_swap.wait_send()
    lax.fori_loop(0, WHOLE + 1, step, 0)
    last = range(WHOLE + 1, SLOTS + 1)
    landed(kv.at[pl.ds(WHOLE + 1, 2), :, :, :, low], recv_sem.at[WHOLE])
    attend(last, 0, t // 2)
    finish(0, nb // 2)
    landed(kv.at[pl.ds(WHOLE + 1, 2), :, :, :, high], recv_sem.at[WHOLE + 1])
    attend(last, t // 2, t)
    finish(nb // 2, nb)
    landed(kv.at[pl.ds(1, SLOTS)], send_sem.at[0])
    landed(ost, out_sem.at[0])
    landed(o_ref.at[:, pl.ds(hh * oz, hh)], out_sem.at[1])


def solution(mesh):
    assert mesh.shape["cx"] == RING and mesh.shape["cy"] == RING and mesh.shape["cz"] == 2
    spec = P(("dp", "cx", "cy", "cz"))

    def local(q, k, v):
        t, hq, d = q.shape
        hkv = k.shape[1]
        g = hq // hkv
        hh = hkv // 2
        nb = t // 16
        w = 2 * 16 * g
        units = SLOTS + 1
        o = pl.pallas_call(
            _kernel,
            out_shape=jax.ShapeDtypeStruct((t, hkv, g, d), jnp.bfloat16),
            in_specs=[pl.BlockSpec(memory_space=pltpu.HBM)] * 3,
            out_specs=pl.BlockSpec(memory_space=pltpu.VMEM),
            scratch_shapes=[
                pltpu.VMEM((t, hkv, d), jnp.bfloat16),
                pltpu.VMEM((t, hkv, d), jnp.bfloat16),
                pltpu.VMEM((hkv, 2, t, d), jnp.bfloat16),
                pltpu.VMEM((units, hh, 2, 2, t, d), jnp.bfloat16),
                pltpu.VMEM((2, t, hh, g, d), jnp.bfloat16),
                pltpu.VMEM((hh, nb, 2, d, 16 * g), jnp.bfloat16),
                pltpu.VMEM((hh, nb, d, w), jnp.float32),
                pltpu.VMEM((hh, nb, 1, w), jnp.float32),
                pltpu.VMEM((hh, nb, 8, w), jnp.float32),
                pltpu.VMEM((hh, t, g, d), jnp.bfloat16),
                pltpu.VMEM((2, nb, 2 * t, w), jnp.float32),
                pltpu.SMEM((units, hh), jnp.int32),
                pltpu.SemaphoreType.DMA((3,)),
                pltpu.SemaphoreType.DMA((4,)),
                pltpu.SemaphoreType.DMA((1,)),
                pltpu.SemaphoreType.DMA((SLOTS,)),
                pltpu.SemaphoreType.DMA((2,)),
            ],
            compiler_params=pltpu.CompilerParams(collective_id=0, has_side_effects=True, vmem_limit_bytes=20 << 20),
        )(*(pltpu.with_memory_space_constraint(x, pltpu.HBM) for x in (k, v, q.reshape(t, hkv, g, d))))
        return o.reshape(t, hq, d)

    return jax.shard_map(local, mesh=mesh, in_specs=(spec, spec, spec), out_specs=spec, check_vma=False)
```

```python
import functools
import math

import jax
import jax.numpy as jnp
from jax import lax
from jax.experimental import pallas as pl
from jax.experimental.pallas import tpu as pltpu
from jax.sharding import PartitionSpec as P

NEG = -1e30
RING = 4
LINKS = (("x", 1), ("x", -1), ("y", 1), ("y", -1))
HEAD_OF = {("x", 1): 0, ("x", -1): 1, ("y", 1): 2, ("y", -1): 3}
PLAN = (
    ("a", -1), ("b", -1), ("c", -1), ("d", -1), ("a", 0), ("c", 0), ("c", 1), ("d", 1),
    ("c", 4), ("c", 2), ("c", 5), ("c", 6), ("d", 0), ("c", 8), ("d", 4),
)
SLOTS = len(PLAN)
AHEAD = 4
WHOLE = SLOTS - 2
LAG = 2


def _head(link, letter):
    axis, sign = link
    other = "y" if axis == "x" else "x"
    return HEAD_OF[{"a": (axis, sign), "b": (axis, -sign), "c": (other, sign), "d": (other, -sign)}[letter]]


def _offsets():
    off = [dict() for _ in range(SLOTS)]
    for slot, (letter, src) in enumerate(PLAN):
        for link in LINKS:
            head = _head(link, letter)
            x, y = (0, 0) if src < 0 else off[src][head]
            axis, sign = link
            x, y = (x + sign, y) if axis == "x" else (x, y + sign)
            assert head not in off[slot]
            off[slot][head] = (x % RING, y % RING)
    for head in range(len(LINKS)):
        assert len({off[s][head] for s in range(SLOTS)} | {(0, 0)}) == RING * RING
    return off


OFF = _offsets()


def _kernel(k_hbm, v_hbm, q_hbm, o_ref, kin, vin, st, kv, qs, qt, acc, m_ref, l_ref, ost, sc, src,
            in_sem, x_sem, send_sem, recv_sem, out_sem):
    t, hkv, d = k_hbm.shape
    g = q_hbm.shape[2]
    hh = hkv // 2
    nb = t // 16
    w = 2 * 16 * g
    iy, ix, iz = lax.axis_index("cx"), lax.axis_index("cy"), lax.axis_index("cz")
    oz = 1 - iz
    chip = iy * RING + ix
    c = d ** -0.5 * math.log2(math.e)

    def peer(link):
        axis, sign = link
        if axis == "x":
            return {"cy": lax.rem(ix + sign + RING, RING)}
        return {"cx": lax.rem(iy + sign + RING, RING)}

    low, high = slice(0, t // 2), slice(t // 2, t)

    k_in = pltpu.make_async_copy(k_hbm, kin, in_sem.at[0])
    v_in = pltpu.make_async_copy(v_hbm, vin, in_sem.at[1])
    q_in = pltpu.make_async_copy(q_hbm.at[:, pl.ds(hh * iz, hh)], qs.at[iz], in_sem.at[2])
    k_in.start()
    v_in.start()
    q_in.start()
    barrier = pltpu.get_barrier_semaphore()
    for link in LINKS:
        pl.semaphore_signal(barrier, inc=1, device_id=peer(link), device_id_type=pl.DeviceIdType.MESH)
    pl.semaphore_signal(barrier, inc=1, device_id={"cz": oz}, device_id_type=pl.DeviceIdType.MESH)

    for n, (ref, copy) in enumerate(((kin, k_in), (vin, v_in))):
        copy.wait()
        x = jnp.swapaxes(ref[...].astype(jnp.float32), 0, 1)
        st[:, n] = x.astype(jnp.bfloat16)
    for h in range(hh):
        kv[0, h, :, iz] = st[hh * iz + h]

    def remote(a, b, s, r, to):
        return pltpu.make_async_remote_copy(
            src_ref=a, dst_ref=b, send_sem=s, recv_sem=r, device_id=to, device_id_type=pl.DeviceIdType.MESH)

    def unit(n, slot, part=0):
        link = LINKS[n]
        letter, arrival = PLAN[slot]
        h = _head(link, letter)
        here, there, to = kv.at[1 + arrival, h], kv.at[1 + slot, h], slot
        if slot < 2:
            z = (iz, oz)[part]
            here, there = (kv.at[0, h, :, z] if part else st.at[hh * iz + h]), there.at[:, z]
        elif slot >= WHOLE:
            rows, to = (low, high)[part], WHOLE + part
            here, there = here.at[:, :, rows], there.at[:, :, rows]
        return remote(here, there, send_sem.at[0], recv_sem.at[to], peer(link))

    def landed(ref, sem):
        pltpu.make_async_copy(ref, ref, sem).wait()

    swap = remote(st.at[pl.ds(hh * oz, hh)], kv.at[0, :, :, iz], x_sem.at[0], x_sem.at[1], {"cz": oz})
    q_swap = remote(q_hbm.at[:, pl.ds(hh * oz, hh)], qs.at[iz], x_sem.at[2], x_sem.at[3], {"cz": oz})

    pl.semaphore_wait(barrier, len(LINKS) + 1)
    swap.start()
    for slot in range(2):
        for n in range(4):
            unit(n, slot).start()
    q_swap.start()
    swap.wait_recv()
    for slot in range(2):
        for n in range(4):
            unit(n, slot, 1).start()
    for slot in range(2, AHEAD):
        for n in range(4):
            unit(n, slot).start()

    m_ref[...] = jnp.full_like(m_ref, NEG)
    l_ref[...] = jnp.zeros_like(l_ref)
    acc[...] = jnp.zeros_like(acc)

    def turn(p):
        @pl.loop(0, hh)
        def _(h):
            for a in range(nb):
                x = qs[p, 16 * a:16 * (a + 1), h].astype(jnp.float32).reshape(16 * g, d)
                qt[h, a, p] = x.T.astype(jnp.bfloat16)

    q_in.wait()
    q_swap.wait_recv()
    for p in range(2):
        turn(p)

    def origin(slot):
        for h in range(hh):
            ox, oy = OFF[slot][h]
            src[slot + 1, h] = lax.rem(iy - oy + RING, RING) * RING + lax.rem(ix - ox + RING, RING)

    lane = lax.broadcasted_iota(jnp.int32, (16, w), 1)
    row = lax.broadcasted_iota(jnp.int32, (16, w), 0)
    lead = lax.rem(lane, w // 2) // g - row

    def attend(units, r0, r1, ahead=2):
        first = r0 // 16
        pieces = [(k, z) for k in units for z in range(2)]

        def scores(h, a):
            n = min(r1, 16 * (a + 1)) - r0
            q = jnp.concatenate([qt[h, a, 0], qt[h, a, 1]], axis=1)
            keys = jnp.concatenate([kv[k, h, 0, z, r0:r0 + n] for k, z in pieces], axis=0)
            sc[h, a, :len(pieces) * n] = jnp.dot(keys, q, preferred_element_type=jnp.float32)

        def weigh(h):
            vis = []
            for k, z in pieces:
                gap = 2 * (chip - src[k, h]) - z
                late = [jnp.where(gap + p >= 0, 0, 1) for p in range(2)]
                vis.append(lead >= jnp.where(lane < w // 2, late[0], late[1]))
            vt = jnp.concatenate([kv[k, h, 1, z, r0:r1] for k, z in pieces], axis=0).T
            for a in range(first, nb):
                n = min(r1, 16 * (a + 1)) - r0
                s = []
                for i in range(len(pieces)):
                    x = sc[h, a, i * n:(i + 1) * n]
                    if 16 * (a + 1) <= r1:
                        edge = jnp.where(vis[i], x[n - 16:], NEG)
                        x = jnp.concatenate([x[:n - 16], edge], axis=0) if n > 16 else edge
                    s.append(x)
                old = m_ref[h, a]
                new = jnp.maximum(old, jnp.max(functools.reduce(jnp.maximum, s), axis=0, keepdims=True))
                m_ref[h, a] = new
                fade = jnp.exp2((old - new) * c)
                top = new * c
                e = [jnp.exp2(x * c - top) for x in s]
                l_ref[h, a] = l_ref[h, a] * fade + jnp.sum(sum(e[1:], e[0]).reshape(n // 8, 8, w), axis=0)
                weights = []
                for x in e:
                    weights.append(x.astype(jnp.bfloat16))
                    if n < r1 - r0:
                        weights.append(jnp.zeros((r1 - r0 - n, w), jnp.bfloat16))
                pv = jnp.dot(vt, jnp.concatenate(weights, axis=0), preferred_element_type=jnp.float32)
                acc[h, a] = acc[h, a] * fade + pv

        for i in range(hh + ahead):
            if i < hh:
                for a in range(first, nb):
                    scores(i, a)
            if i >= ahead:
                weigh(i - ahead)

    def out(h, rows):
        return remote(ost.at[h, rows], o_ref.at[rows, hh * iz + h], out_sem.at[0], out_sem.at[1], {"cz": oz})

    def finish(a0, a1):
        @pl.loop(0, hh)
        def _(h):
            for a in range(a0, a1):
                o = (acc[h, a] * (1.0 / jnp.sum(l_ref[h, a], axis=0, keepdims=True))).astype(jnp.bfloat16)
                x = [o[:, p * 16 * g:(p + 1) * 16 * g].T.reshape(16, g, d) for p in range(2)]
                here = iz == 0
                ost[h, 16 * a:16 * (a + 1)] = jnp.where(here, x[1], x[0])
                o_ref[16 * a:16 * (a + 1), hh * iz + h] = jnp.where(here, x[0], x[1])
            out(h, slice(16 * a0, 16 * a1)).start()

    def send_last(part):
        for slot in range(WHOLE, SLOTS):
            for n in range(4):
                unit(n, slot, part).start()

    def step(k, carry):
        for j in range(1, WHOLE + 1):
            @pl.when(k == j)
            def _():
                landed(kv.at[j], recv_sem.at[j - 1])
                if j - 1 + AHEAD < WHOLE:
                    for n in range(4):
                        unit(n, j - 1 + AHEAD).start()
                if j - 1 + AHEAD == WHOLE:
                    send_last(0)
                if j - 1 + AHEAD == WHOLE + 1:
                    @pl.when(iz == 0)
                    def _():
                        send_last(1)
                if j == SLOTS - LAG:
                    @pl.when(iz == 1)
                    def _():
                        send_last(1)
        attend((k,), 0, t)
        return carry

    for h in range(hh):
        src[0, h] = chip
    for slot in range(SLOTS):
        origin(slot)
    swap.wait_send()
    q_swap.wait_send()
    lax.fori_loop(0, WHOLE + 1, step, 0)
    last = range(WHOLE + 1, SLOTS + 1)
    landed(kv.at[pl.ds(WHOLE + 1, 2), :, :, :, low], recv_sem.at[WHOLE])
    attend(last, 0, t // 2)
    finish(0, nb // 2)
    landed(kv.at[pl.ds(WHOLE + 1, 2), :, :, :, high], recv_sem.at[WHOLE + 1])
    attend(last, t // 2, t, 2)
    finish(nb // 2, nb)
    landed(kv.at[pl.ds(1, SLOTS)], send_sem.at[0])
    landed(ost, out_sem.at[0])
    landed(o_ref.at[:, pl.ds(hh * oz, hh)], out_sem.at[1])


def solution(mesh):
    assert mesh.shape["cx"] == RING and mesh.shape["cy"] == RING and mesh.shape["cz"] == 2
    spec = P(("dp", "cx", "cy", "cz"))

    def local(q, k, v):
        t, hq, d = q.shape
        hkv = k.shape[1]
        g = hq // hkv
        hh = hkv // 2
        nb = t // 16
        w = 2 * 16 * g
        units = SLOTS + 1
        o = pl.pallas_call(
            _kernel,
            out_shape=jax.ShapeDtypeStruct((t, hkv, g, d), jnp.bfloat16),
            in_specs=[pl.BlockSpec(memory_space=pltpu.HBM)] * 3,
            out_specs=pl.BlockSpec(memory_space=pltpu.VMEM),
            scratch_shapes=[
                pltpu.VMEM((t, hkv, d), jnp.bfloat16),
                pltpu.VMEM((t, hkv, d), jnp.bfloat16),
                pltpu.VMEM((hkv, 2, t, d), jnp.bfloat16),
                pltpu.VMEM((units, hh, 2, 2, t, d), jnp.bfloat16),
                pltpu.VMEM((2, t, hh, g, d), jnp.bfloat16),
                pltpu.VMEM((hh, nb, 2, d, 16 * g), jnp.bfloat16),
                pltpu.VMEM((hh, nb, d, w), jnp.float32),
                pltpu.VMEM((hh, nb, 1, w), jnp.float32),
                pltpu.VMEM((hh, nb, 8, w), jnp.float32),
                pltpu.VMEM((hh, t, g, d), jnp.bfloat16),
                pltpu.VMEM((hh, nb, 2 * t, w), jnp.float32),
                pltpu.SMEM((units, hh), jnp.int32),
                pltpu.SemaphoreType.DMA((3,)),
                pltpu.SemaphoreType.DMA((4,)),
                pltpu.SemaphoreType.DMA((1,)),
                pltpu.SemaphoreType.DMA((SLOTS,)),
                pltpu.SemaphoreType.DMA((2,)),
            ],
            compiler_params=pltpu.CompilerParams(collective_id=0, has_side_effects=True, vmem_limit_bytes=20 << 20),
        )(*(pltpu.with_memory_space_constraint(x, pltpu.HBM) for x in (k, v, q.reshape(t, hkv, g, d))))
        return o.reshape(t, hq, d)

    return jax.shard_map(local, mesh=mesh, in_specs=(spec, spec, spec), out_specs=spec, check_vma=False)
```

```python
import functools
import math

import jax
import jax.numpy as jnp
from jax import lax
from jax.experimental import pallas as pl
from jax.experimental.pallas import tpu as pltpu
from jax.sharding import PartitionSpec as P

NEG = -1e30
RING = 4
LINKS = (("x", 1), ("x", -1), ("y", 1), ("y", -1))
HEAD_OF = {("x", 1): 0, ("x", -1): 1, ("y", 1): 2, ("y", -1): 3}
PLAN = (
    ("a", -1), ("b", -1), ("c", -1), ("d", -1), ("a", 0), ("c", 0), ("c", 1), ("d", 1),
    ("c", 4), ("c", 2), ("c", 5), ("c", 6), ("d", 0), ("c", 8), ("d", 4),
)
SLOTS = len(PLAN)
AHEAD = 4
RECVS = 2 * AHEAD
WHOLE = SLOTS - 2
LAG = 2


def _head(link, letter):
    axis, sign = link
    other = "y" if axis == "x" else "x"
    return HEAD_OF[{"a": (axis, sign), "b": (axis, -sign), "c": (other, sign), "d": (other, -sign)}[letter]]


def _offsets():
    off = [dict() for _ in range(SLOTS)]
    for slot, (letter, src) in enumerate(PLAN):
        for link in LINKS:
            head = _head(link, letter)
            x, y = (0, 0) if src < 0 else off[src][head]
            axis, sign = link
            x, y = (x + sign, y) if axis == "x" else (x, y + sign)
            assert head not in off[slot]
            off[slot][head] = (x % RING, y % RING)
    for head in range(len(LINKS)):
        assert len({off[s][head] for s in range(SLOTS)} | {(0, 0)}) == RING * RING
    return off


OFF = _offsets()


def _kernel(k_hbm, v_hbm, q_hbm, o_ref, kin, vin, st, kv, qs, qt, acc, m_ref, l_ref, ost, sc, src,
            in_sem, x_sem, send_sem, recv_sem, out_sem):
    t, hkv, d = k_hbm.shape
    g = q_hbm.shape[2]
    hh = hkv // 2
    nb = t // 16
    w = 2 * 16 * g
    iy, ix, iz = lax.axis_index("cx"), lax.axis_index("cy"), lax.axis_index("cz")
    oz = 1 - iz
    chip = iy * RING + ix
    c = d ** -0.5 * math.log2(math.e)

    def peer(link):
        axis, sign = link
        if axis == "x":
            return {"cy": lax.rem(ix + sign + RING, RING)}
        return {"cx": lax.rem(iy + sign + RING, RING)}

    low, high = slice(0, t // 2), slice(t // 2, t)

    k_in = pltpu.make_async_copy(k_hbm, kin, in_sem.at[0])
    v_in = pltpu.make_async_copy(v_hbm, vin, in_sem.at[1])
    q_in = pltpu.make_async_copy(q_hbm.at[:, pl.ds(hh * iz, hh)], qs.at[iz], in_sem.at[2])
    k_in.start()
    v_in.start()
    q_in.start()
    barrier = pltpu.get_barrier_semaphore()
    for link in LINKS:
        pl.semaphore_signal(barrier, inc=1, device_id=peer(link), device_id_type=pl.DeviceIdType.MESH)
    pl.semaphore_signal(barrier, inc=1, device_id={"cz": oz}, device_id_type=pl.DeviceIdType.MESH)

    for n, (ref, copy) in enumerate(((kin, k_in), (vin, v_in))):
        copy.wait()
        x = jnp.swapaxes(ref[...].astype(jnp.float32), 0, 1)
        st[:, n] = x.astype(jnp.bfloat16)

    def remote(a, b, s, r, to):
        return pltpu.make_async_remote_copy(
            src_ref=a, dst_ref=b, send_sem=s, recv_sem=r, device_id=to, device_id_type=pl.DeviceIdType.MESH)

    def unit(n, slot, part=0):
        link = LINKS[n]
        letter, arrival = PLAN[slot]
        h = _head(link, letter)
        here, there, to = kv.at[1 + arrival, h], kv.at[1 + slot, h], slot
        if slot < 2:
            z = (iz, oz)[part]
            here, there = (kv.at[0, h, :, z] if part else st.at[hh * iz + h]), there.at[:, z]
        elif slot >= WHOLE:
            rows, to = (low, high)[part], WHOLE + part
            here, there = here.at[:, :, rows], there.at[:, :, rows]
        return remote(here, there, send_sem.at[0], recv_sem.at[to % RECVS], peer(link))

    def landed(ref, sem):
        pltpu.make_async_copy(ref, ref, sem).wait()

    swap = remote(st.at[pl.ds(hh * oz, hh)], kv.at[0, :, :, iz], x_sem.at[0], x_sem.at[1], {"cz": oz})
    q_swap = remote(q_hbm.at[:, pl.ds(hh * oz, hh)], qs.at[iz], x_sem.at[2], x_sem.at[3], {"cz": oz})

    pl.semaphore_wait(barrier, len(LINKS) + 1)
    for n in range(4):
        unit(n, 0).start()
    swap.start()
    for n in range(4):
        unit(n, 1).start()
    for h in range(hh):
        kv[0, h, :, iz] = st[hh * iz + h]
    q_swap.start()
    swap.wait_recv()
    for slot in range(2):
        for n in range(4):
            unit(n, slot, 1).start()
    for slot in range(2, AHEAD):
        for n in range(4):
            unit(n, slot).start()

    m_ref[...] = jnp.full_like(m_ref, NEG)
    l_ref[...] = jnp.zeros_like(l_ref)
    acc[...] = jnp.zeros_like(acc)

    def turn(p):
        @pl.loop(0, hh)
        def _(h):
            for a in range(nb):
                x = qs[p, 16 * a:16 * (a + 1), h].astype(jnp.float32).reshape(16 * g, d)
                qt[h, a, p] = x.T.astype(jnp.bfloat16)

    q_in.wait()
    q_swap.wait_recv()
    for p in range(2):
        turn(p)

    def origin(slot):
        for h in range(hh):
            ox, oy = OFF[slot][h]
            src[slot + 1, h] = lax.rem(iy - oy + RING, RING) * RING + lax.rem(ix - ox + RING, RING)

    lane = lax.broadcasted_iota(jnp.int32, (16, w), 1)
    row = lax.broadcasted_iota(jnp.int32, (16, w), 0)
    lead = lax.rem(lane, w // 2) // g - row

    def attend(units, r0, r1, ahead=2):
        first = r0 // 16
        pieces = [(k, z) for k in units for z in range(2)]

        def scores(h, a):
            n = min(r1, 16 * (a + 1)) - r0
            q = jnp.concatenate([qt[h, a, 0], qt[h, a, 1]], axis=1)
            keys = jnp.concatenate([kv[k, h, 0, z, r0:r0 + n] for k, z in pieces], axis=0)
            sc[h, a, :len(pieces) * n] = jnp.dot(keys, q, preferred_element_type=jnp.float32)

        def weigh(h):
            vis = []
            for k, z in pieces:
                gap = 2 * (chip - src[k, h]) - z
                late = [jnp.where(gap + p >= 0, 0, 1) for p in range(2)]
                vis.append(lead >= jnp.where(lane < w // 2, late[0], late[1]))
            vt = jnp.concatenate([kv[k, h, 1, z, r0:r1] for k, z in pieces], axis=0).T
            for a in range(first, nb):
                n = min(r1, 16 * (a + 1)) - r0
                s = []
                for i in range(len(pieces)):
                    x = sc[h, a, i * n:(i + 1) * n]
                    if 16 * (a + 1) <= r1:
                        edge = jnp.where(vis[i], x[n - 16:], NEG)
                        x = jnp.concatenate([x[:n - 16], edge], axis=0) if n > 16 else edge
                    s.append(x)
                old = m_ref[h, a]
                new = jnp.maximum(old, jnp.max(functools.reduce(jnp.maximum, s), axis=0, keepdims=True))
                m_ref[h, a] = new
                fade = jnp.exp2((old - new) * c)
                top = new * c
                e = [jnp.exp2(x * c - top) for x in s]
                l_ref[h, a] = l_ref[h, a] * fade + jnp.sum(sum(e[1:], e[0]).reshape(n // 8, 8, w), axis=0)
                weights = []
                for x in e:
                    weights.append(x.astype(jnp.bfloat16))
                    if n < r1 - r0:
                        weights.append(jnp.zeros((r1 - r0 - n, w), jnp.bfloat16))
                pv = jnp.dot(vt, jnp.concatenate(weights, axis=0), preferred_element_type=jnp.float32)
                acc[h, a] = acc[h, a] * fade + pv

        for i in range(hh + ahead):
            if i < hh:
                for a in range(first, nb):
                    scores(i, a)
            if i >= ahead:
                weigh(i - ahead)

    def out(h, rows):
        return remote(ost.at[h, rows], o_ref.at[rows, hh * iz + h], out_sem.at[0], out_sem.at[1], {"cz": oz})

    def finish(a0, a1):
        @pl.loop(0, hh)
        def _(h):
            for a in range(a0, a1):
                o = (acc[h, a] * (1.0 / jnp.sum(l_ref[h, a], axis=0, keepdims=True))).astype(jnp.bfloat16)
                x = [o[:, p * 16 * g:(p + 1) * 16 * g].T.reshape(16, g, d) for p in range(2)]
                here = iz == 0
                ost[h, 16 * a:16 * (a + 1)] = jnp.where(here, x[1], x[0])
                o_ref[16 * a:16 * (a + 1), hh * iz + h] = jnp.where(here, x[0], x[1])
            out(h, slice(16 * a0, 16 * a1)).start()

    def send_last(part):
        for slot in range(WHOLE, SLOTS):
            for n in range(4):
                unit(n, slot, part).start()

    def step(k, carry):
        for j in range(1, WHOLE + 1):
            @pl.when(k == j)
            def _():
                landed(kv.at[j], recv_sem.at[(j - 1) % RECVS])
                if j - 1 + AHEAD < WHOLE:
                    for n in range(4):
                        unit(n, j - 1 + AHEAD).start()
                if j - 1 + AHEAD == WHOLE:
                    send_last(0)
                if j - 1 + AHEAD == WHOLE + 1:
                    @pl.when(iz == 0)
                    def _():
                        send_last(1)
                if j == SLOTS - LAG:
                    @pl.when(iz == 1)
                    def _():
                        send_last(1)
        attend((k,), 0, t)
        return carry

    for h in range(hh):
        src[0, h] = chip
    for slot in range(SLOTS):
        origin(slot)
    swap.wait_send()
    q_swap.wait_send()
    lax.fori_loop(0, WHOLE + 1, step, 0)
    last = range(WHOLE + 1, SLOTS + 1)
    landed(kv.at[pl.ds(WHOLE + 1, 2), :, :, :, low], recv_sem.at[WHOLE % RECVS])
    attend(last, 0, t // 2)
    finish(0, nb // 2)
    landed(kv.at[pl.ds(WHOLE + 1, 2), :, :, :, high], recv_sem.at[(WHOLE + 1) % RECVS])
    attend(last, t // 2, t, 2)
    finish(nb // 2, nb)
    landed(kv.at[pl.ds(1, SLOTS)], send_sem.at[0])
    landed(ost, out_sem.at[0])
    landed(o_ref.at[:, pl.ds(hh * oz, hh)], out_sem.at[1])


def solution(mesh):
    assert mesh.shape["cx"] == RING and mesh.shape["cy"] == RING and mesh.shape["cz"] == 2
    spec = P(("dp", "cx", "cy", "cz"))

    def local(q, k, v):
        t, hq, d = q.shape
        hkv = k.shape[1]
        g = hq // hkv
        hh = hkv // 2
        nb = t // 16
        w = 2 * 16 * g
        units = SLOTS + 1
        o = pl.pallas_call(
            _kernel,
            out_shape=jax.ShapeDtypeStruct((t, hkv, g, d), jnp.bfloat16),
            in_specs=[pl.BlockSpec(memory_space=pltpu.HBM)] * 3,
            out_specs=pl.BlockSpec(memory_space=pltpu.VMEM),
            scratch_shapes=[
                pltpu.VMEM((t, hkv, d), jnp.bfloat16),
                pltpu.VMEM((t, hkv, d), jnp.bfloat16),
                pltpu.VMEM((hkv, 2, t, d), jnp.bfloat16),
                pltpu.VMEM((units, hh, 2, 2, t, d), jnp.bfloat16),
                pltpu.VMEM((2, t, hh, g, d), jnp.bfloat16),
                pltpu.VMEM((hh, nb, 2, d, 16 * g), jnp.bfloat16),
                pltpu.VMEM((hh, nb, d, w), jnp.float32),
                pltpu.VMEM((hh, nb, 1, w), jnp.float32),
                pltpu.VMEM((hh, nb, 8, w), jnp.float32),
                pltpu.VMEM((hh, t, g, d), jnp.bfloat16),
                pltpu.VMEM((hh, nb, 2 * t, w), jnp.float32),
                pltpu.SMEM((units, hh), jnp.int32),
                pltpu.SemaphoreType.DMA((3,)),
                pltpu.SemaphoreType.DMA((4,)),
                pltpu.SemaphoreType.DMA((1,)),
                pltpu.SemaphoreType.DMA((RECVS,)),
                pltpu.SemaphoreType.DMA((2,)),
            ],
            compiler_params=pltpu.CompilerParams(collective_id=0, has_side_effects=True, vmem_limit_bytes=20 << 20),
        )(*(pltpu.with_memory_space_constraint(x, pltpu.HBM) for x in (k, v, q.reshape(t, hkv, g, d))))
        return o.reshape(t, hq, d)

    return jax.shard_map(local, mesh=mesh, in_specs=(spec, spec, spec), out_specs=spec, check_vma=False)
```

```python
import functools
import math

import jax
import jax.numpy as jnp
from jax import lax
from jax.experimental import pallas as pl
from jax.experimental.pallas import tpu as pltpu
from jax.sharding import PartitionSpec as P

NEG = -1e30
RING = 4
LINKS = (("x", 1), ("x", -1), ("y", 1), ("y", -1))
HEAD_OF = {("x", 1): 0, ("x", -1): 1, ("y", 1): 2, ("y", -1): 3}
PLAN = (
    ("a", -1), ("b", -1), ("c", -1), ("d", -1), ("a", 0), ("c", 0), ("c", 1), ("d", 1),
    ("c", 4), ("c", 2), ("c", 5), ("c", 6), ("d", 0), ("c", 8), ("d", 4),
)
SLOTS = len(PLAN)
AHEAD = 4
RECVS = 2 * AHEAD
WHOLE = SLOTS - 2
LAG = 2


def _head(link, letter):
    axis, sign = link
    other = "y" if axis == "x" else "x"
    return HEAD_OF[{"a": (axis, sign), "b": (axis, -sign), "c": (other, sign), "d": (other, -sign)}[letter]]


def _offsets():
    off = [dict() for _ in range(SLOTS)]
    for slot, (letter, src) in enumerate(PLAN):
        for link in LINKS:
            head = _head(link, letter)
            x, y = (0, 0) if src < 0 else off[src][head]
            axis, sign = link
            x, y = (x + sign, y) if axis == "x" else (x, y + sign)
            assert head not in off[slot]
            off[slot][head] = (x % RING, y % RING)
    for head in range(len(LINKS)):
        assert len({off[s][head] for s in range(SLOTS)} | {(0, 0)}) == RING * RING
    return off


OFF = _offsets()


def _kernel(k_hbm, v_hbm, q_hbm, o_ref, kin, vin, st, kv, qs, qt, acc, m_ref, l_ref, ost, sc, src,
            in_sem, x_sem, send_sem, recv_sem, out_sem):
    t, hkv, d = k_hbm.shape
    g = q_hbm.shape[2]
    hh = hkv // 2
    nb = t // 16
    w = 2 * 16 * g
    iy, ix, iz = lax.axis_index("cx"), lax.axis_index("cy"), lax.axis_index("cz")
    oz = 1 - iz
    chip = iy * RING + ix
    c = d ** -0.5 * math.log2(math.e)

    def peer(link):
        axis, sign = link
        if axis == "x":
            return {"cy": lax.rem(ix + sign + RING, RING)}
        return {"cx": lax.rem(iy + sign + RING, RING)}

    low, high = slice(0, t // 2), slice(t // 2, t)

    k_in = pltpu.make_async_copy(k_hbm, kin, in_sem.at[0])
    v_in = pltpu.make_async_copy(v_hbm, vin, in_sem.at[1])
    q_in = pltpu.make_async_copy(q_hbm.at[:, pl.ds(hh * iz, hh)], qs.at[iz], in_sem.at[2])
    k_in.start()
    v_in.start()
    q_in.start()
    barrier = pltpu.get_barrier_semaphore()
    for link in LINKS:
        pl.semaphore_signal(barrier, inc=1, device_id=peer(link), device_id_type=pl.DeviceIdType.MESH)
    pl.semaphore_signal(barrier, inc=1, device_id={"cz": oz}, device_id_type=pl.DeviceIdType.MESH)

    for n, (ref, copy) in enumerate(((kin, k_in), (vin, v_in))):
        copy.wait()
        x = jnp.swapaxes(ref[...].astype(jnp.float32), 0, 1)
        st[:, n] = x.astype(jnp.bfloat16)

    def remote(a, b, s, r, to):
        return pltpu.make_async_remote_copy(
            src_ref=a, dst_ref=b, send_sem=s, recv_sem=r, device_id=to, device_id_type=pl.DeviceIdType.MESH)

    def unit(n, slot, part=0):
        link = LINKS[n]
        letter, arrival = PLAN[slot]
        h = _head(link, letter)
        here, there, to = kv.at[1 + arrival, h], kv.at[1 + slot, h], slot
        if slot < 2:
            z = (iz, oz)[part]
            here, there = (kv.at[0, h, :, z] if part else st.at[hh * iz + h]), there.at[:, z]
        elif slot >= WHOLE:
            rows, to = (low, high)[part], WHOLE + part
            here, there = here.at[:, :, rows], there.at[:, :, rows]
        return remote(here, there, send_sem.at[0], recv_sem.at[to % RECVS], peer(link))

    def landed(ref, sem):
        pltpu.make_async_copy(ref, ref, sem).wait()

    swap = remote(st.at[pl.ds(hh * oz, hh)], kv.at[0, :, :, iz], x_sem.at[0], x_sem.at[1], {"cz": oz})
    q_swap = remote(q_hbm.at[:, pl.ds(hh * oz, hh)], qs.at[iz], x_sem.at[2], x_sem.at[3], {"cz": oz})

    pl.semaphore_wait(barrier, len(LINKS) + 1)
    for n in range(4):
        unit(n, 0).start()
    swap.start()
    for n in range(4):
        unit(n, 1).start()
    for h in range(hh):
        kv[0, h, :, iz] = st[hh * iz + h]
    q_swap.start()
    swap.wait_recv()
    for slot in range(2):
        for n in range(4):
            unit(n, slot, 1).start()
    for slot in range(2, AHEAD):
        for n in range(4):
            unit(n, slot).start()

    m_ref[...] = jnp.full_like(m_ref, NEG)
    l_ref[...] = jnp.zeros_like(l_ref)
    acc[...] = jnp.zeros_like(acc)

    def turn(p):
        @pl.loop(0, hh)
        def _(h):
            for a in range(nb):
                x = qs[p, 16 * a:16 * (a + 1), h].astype(jnp.float32).reshape(16 * g, d)
                qt[h, a, p] = x.T.astype(jnp.bfloat16)

    q_in.wait()
    q_swap.wait_recv()
    for p in range(2):
        turn(p)

    def origin(slot):
        for h in range(hh):
            ox, oy = OFF[slot][h]
            src[slot + 1, h] = lax.rem(iy - oy + RING, RING) * RING + lax.rem(ix - ox + RING, RING)

    lane = lax.broadcasted_iota(jnp.int32, (16, w), 1)
    row = lax.broadcasted_iota(jnp.int32, (16, w), 0)
    lead = lax.rem(lane, w // 2) // g - row

    def attend(units, r0, r1, ahead=2):
        first = r0 // 16
        pieces = [(k, z) for k in units for z in range(2)]

        def scores(h, a):
            n = min(r1, 16 * (a + 1)) - r0
            q = jnp.concatenate([qt[h, a, 0], qt[h, a, 1]], axis=1)
            keys = jnp.concatenate([kv[k, h, 0, z, r0:r0 + n] for k, z in pieces], axis=0)
            sc[h, a, :len(pieces) * n] = jnp.dot(keys, q, preferred_element_type=jnp.float32)

        def weigh(h):
            vis = []
            for k, z in pieces:
                gap = 2 * (chip - src[k, h]) - z
                late = [jnp.where(gap + p >= 0, 0, 1) for p in range(2)]
                vis.append(lead >= jnp.where(lane < w // 2, late[0], late[1]))
            vt = jnp.concatenate([kv[k, h, 1, z, r0:r1] for k, z in pieces], axis=0).T
            for a in range(first, nb):
                n = min(r1, 16 * (a + 1)) - r0
                s = []
                for i in range(len(pieces)):
                    x = sc[h, a, i * n:(i + 1) * n]
                    if 16 * (a + 1) <= r1:
                        edge = jnp.where(vis[i], x[n - 16:], NEG)
                        x = jnp.concatenate([x[:n - 16], edge], axis=0) if n > 16 else edge
                    s.append(x)
                old = m_ref[h, a]
                new = jnp.maximum(old, jnp.max(functools.reduce(jnp.maximum, s), axis=0, keepdims=True))
                m_ref[h, a] = new
                fade = jnp.exp2((old - new) * c)
                top = new * c
                e = [jnp.exp2(x * c - top) for x in s]
                l_ref[h, a] = l_ref[h, a] * fade + jnp.sum(sum(e[1:], e[0]).reshape(n // 8, 8, w), axis=0)
                weights = []
                for x in e:
                    weights.append(x.astype(jnp.bfloat16))
                    if n < r1 - r0:
                        weights.append(jnp.zeros((r1 - r0 - n, w), jnp.bfloat16))
                pv = jnp.dot(vt, jnp.concatenate(weights, axis=0), preferred_element_type=jnp.float32)
                acc[h, a] = acc[h, a] * fade + pv

        for i in range(hh + ahead):
            if i < hh:
                for a in range(first, nb):
                    scores(i, a)
            if i >= ahead:
                weigh(i - ahead)

    def out(h, rows):
        return remote(ost.at[h, rows], o_ref.at[rows, hh * iz + h], out_sem.at[0], out_sem.at[1], {"cz": oz})

    def finish(a0, a1, together):
        @pl.loop(0, hh // together)
        def _(i):
            for h in [i * together + n for n in range(together)]:
                for a in range(a0, a1):
                    o = (acc[h, a] * (1.0 / jnp.sum(l_ref[h, a], axis=0, keepdims=True))).astype(jnp.bfloat16)
                    x = [o[:, p * 16 * g:(p + 1) * 16 * g].T.reshape(16, g, d) for p in range(2)]
                    here = iz == 0
                    ost[h, 16 * a:16 * (a + 1)] = jnp.where(here, x[1], x[0])
                    o_ref[16 * a:16 * (a + 1), hh * iz + h] = jnp.where(here, x[0], x[1])
            for h in [i * together + n for n in range(together)]:
                out(h, slice(16 * a0, 16 * a1)).start()

    def send_last(part):
        for slot in range(WHOLE, SLOTS):
            for n in range(4):
                unit(n, slot, part).start()

    def step(k, carry):
        for j in range(1, WHOLE + 1):
            @pl.when(k == j)
            def _():
                landed(kv.at[j], recv_sem.at[(j - 1) % RECVS])
                if j - 1 + AHEAD < WHOLE:
                    for n in range(4):
                        unit(n, j - 1 + AHEAD).start()
                if j - 1 + AHEAD == WHOLE:
                    send_last(0)
                if j - 1 + AHEAD == WHOLE + 1:
                    @pl.when(iz == 0)
                    def _():
                        send_last(1)
                if j == SLOTS - LAG:
                    @pl.when(iz == 1)
                    def _():
                        send_last(1)
        attend((k,), 0, t)
        return carry

    for h in range(hh):
        src[0, h] = chip
    for slot in range(SLOTS):
        origin(slot)
    swap.wait_send()
    q_swap.wait_send()
    lax.fori_loop(0, WHOLE + 1, step, 0)
    last = range(WHOLE + 1, SLOTS + 1)
    landed(kv.at[pl.ds(WHOLE + 1, 2), :, :, :, low], recv_sem.at[WHOLE % RECVS])
    attend(last, 0, t // 2)
    finish(0, nb // 2, 2)
    landed(kv.at[pl.ds(WHOLE + 1, 2), :, :, :, high], recv_sem.at[(WHOLE + 1) % RECVS])
    attend(last, t // 2, t, 2)
    finish(nb // 2, nb, 1)
    landed(kv.at[pl.ds(1, SLOTS)], send_sem.at[0])
    landed(ost, out_sem.at[0])
    landed(o_ref.at[:, pl.ds(hh * oz, hh)], out_sem.at[1])


def solution(mesh):
    assert mesh.shape["cx"] == RING and mesh.shape["cy"] == RING and mesh.shape["cz"] == 2
    spec = P(("dp", "cx", "cy", "cz"))

    def local(q, k, v):
        t, hq, d = q.shape
        hkv = k.shape[1]
        g = hq // hkv
        hh = hkv // 2
        nb = t // 16
        w = 2 * 16 * g
        units = SLOTS + 1
        o = pl.pallas_call(
            _kernel,
            out_shape=jax.ShapeDtypeStruct((t, hkv, g, d), jnp.bfloat16),
            in_specs=[pl.BlockSpec(memory_space=pltpu.HBM)] * 3,
            out_specs=pl.BlockSpec(memory_space=pltpu.VMEM),
            scratch_shapes=[
                pltpu.VMEM((t, hkv, d), jnp.bfloat16),
                pltpu.VMEM((t, hkv, d), jnp.bfloat16),
                pltpu.VMEM((hkv, 2, t, d), jnp.bfloat16),
                pltpu.VMEM((units, hh, 2, 2, t, d), jnp.bfloat16),
                pltpu.VMEM((2, t, hh, g, d), jnp.bfloat16),
                pltpu.VMEM((hh, nb, 2, d, 16 * g), jnp.bfloat16),
                pltpu.VMEM((hh, nb, d, w), jnp.float32),
                pltpu.VMEM((hh, nb, 1, w), jnp.float32),
                pltpu.VMEM((hh, nb, 8, w), jnp.float32),
                pltpu.VMEM((hh, t, g, d), jnp.bfloat16),
                pltpu.VMEM((hh, nb, 2 * t, w), jnp.float32),
                pltpu.SMEM((units, hh), jnp.int32),
                pltpu.SemaphoreType.DMA((3,)),
                pltpu.SemaphoreType.DMA((4,)),
                pltpu.SemaphoreType.DMA((1,)),
                pltpu.SemaphoreType.DMA((RECVS,)),
                pltpu.SemaphoreType.DMA((2,)),
            ],
            compiler_params=pltpu.CompilerParams(collective_id=0, has_side_effects=True, vmem_limit_bytes=20 << 20),
        )(*(pltpu.with_memory_space_constraint(x, pltpu.HBM) for x in (k, v, q.reshape(t, hkv, g, d))))
        return o.reshape(t, hq, d)

    return jax.shard_map(local, mesh=mesh, in_specs=(spec, spec, spec), out_specs=spec, check_vma=False)
```

```python
import functools
import math

import jax
import jax.numpy as jnp
from jax import lax
from jax.experimental import pallas as pl
from jax.experimental.pallas import tpu as pltpu
from jax.sharding import PartitionSpec as P

NEG = -1e30
RING = 4
LINKS = (("x", 1), ("x", -1), ("y", 1), ("y", -1))
HEAD_OF = {("x", 1): 0, ("x", -1): 1, ("y", 1): 2, ("y", -1): 3}
PLAN = (
    ("a", -1), ("b", -1), ("c", -1), ("d", -1), ("a", 0), ("c", 0), ("c", 1), ("d", 1),
    ("c", 4), ("c", 2), ("c", 5), ("c", 6), ("d", 0), ("c", 8), ("d", 4),
)
SLOTS = len(PLAN)
AHEAD = 4
RECVS = 2 * AHEAD
WHOLE = SLOTS - 2
LAG = 2


def _head(link, letter):
    axis, sign = link
    other = "y" if axis == "x" else "x"
    return HEAD_OF[{"a": (axis, sign), "b": (axis, -sign), "c": (other, sign), "d": (other, -sign)}[letter]]


def _offsets():
    off = [dict() for _ in range(SLOTS)]
    for slot, (letter, src) in enumerate(PLAN):
        for link in LINKS:
            head = _head(link, letter)
            x, y = (0, 0) if src < 0 else off[src][head]
            axis, sign = link
            x, y = (x + sign, y) if axis == "x" else (x, y + sign)
            assert head not in off[slot]
            off[slot][head] = (x % RING, y % RING)
    for head in range(len(LINKS)):
        assert len({off[s][head] for s in range(SLOTS)} | {(0, 0)}) == RING * RING
    return off


OFF = _offsets()


def _kernel(k_hbm, v_hbm, q_hbm, o_ref, kin, vin, st, kv, qs, qt, acc, m_ref, l_ref, ost, sc, src,
            in_sem, x_sem, send_sem, recv_sem, out_sem):
    t, hkv, d = k_hbm.shape
    g = q_hbm.shape[2]
    hh = hkv // 2
    nb = t // 16
    w = 2 * 16 * g
    iy, ix, iz = lax.axis_index("cx"), lax.axis_index("cy"), lax.axis_index("cz")
    oz = 1 - iz
    chip = iy * RING + ix
    c = d ** -0.5 * math.log2(math.e)

    def peer(link):
        axis, sign = link
        if axis == "x":
            return {"cy": lax.rem(ix + sign + RING, RING)}
        return {"cx": lax.rem(iy + sign + RING, RING)}

    low, high = slice(0, t // 2), slice(t // 2, t)

    k_in = pltpu.make_async_copy(k_hbm, kin, in_sem.at[0])
    v_in = pltpu.make_async_copy(v_hbm, vin, in_sem.at[1])
    q_in = pltpu.make_async_copy(q_hbm.at[:, pl.ds(hh * iz, hh)], qs.at[iz], in_sem.at[2])
    k_in.start()
    v_in.start()
    q_in.start()
    barrier = pltpu.get_barrier_semaphore()
    for link in LINKS:
        pl.semaphore_signal(barrier, inc=1, device_id=peer(link), device_id_type=pl.DeviceIdType.MESH)
    pl.semaphore_signal(barrier, inc=1, device_id={"cz": oz}, device_id_type=pl.DeviceIdType.MESH)

    for n, (ref, copy) in enumerate(((kin, k_in), (vin, v_in))):
        copy.wait()
        x = jnp.swapaxes(ref[...].astype(jnp.float32), 0, 1)
        st[:, n] = x.astype(jnp.bfloat16)

    def remote(a, b, s, r, to):
        return pltpu.make_async_remote_copy(
            src_ref=a, dst_ref=b, send_sem=s, recv_sem=r, device_id=to, device_id_type=pl.DeviceIdType.MESH)

    def unit(n, slot, part=0):
        link = LINKS[n]
        letter, arrival = PLAN[slot]
        h = _head(link, letter)
        here, there, to = kv.at[1 + arrival, h], kv.at[1 + slot, h], slot
        if slot < 2:
            z = (iz, oz)[part]
            here, there = (kv.at[0, h, :, z] if part else st.at[hh * iz + h]), there.at[:, z]
        elif slot >= WHOLE:
            rows, to = (low, high)[part], WHOLE + part
            here, there = here.at[:, :, rows], there.at[:, :, rows]
        return remote(here, there, send_sem.at[0], recv_sem.at[to % RECVS], peer(link))

    def landed(ref, sem):
        pltpu.make_async_copy(ref, ref, sem).wait()

    swap = remote(st.at[pl.ds(hh * oz, hh)], kv.at[0, :, :, iz], x_sem.at[0], x_sem.at[1], {"cz": oz})
    q_swap = remote(q_hbm.at[:, pl.ds(hh * oz, hh)], qs.at[iz], x_sem.at[2], x_sem.at[3], {"cz": oz})

    pl.semaphore_wait(barrier, len(LINKS) + 1)
    for n in range(4):
        unit(n, 0).start()
    swap.start()
    for n in range(4):
        unit(n, 1).start()
    for h in range(hh):
        kv[0, h, :, iz] = st[hh * iz + h]
    q_swap.start()
    swap.wait_recv()
    for slot in range(2):
        for n in range(4):
            unit(n, slot, 1).start()
    for slot in range(2, AHEAD):
        for n in range(4):
            unit(n, slot).start()

    m_ref[...] = jnp.full_like(m_ref, NEG)
    l_ref[...] = jnp.zeros_like(l_ref)
    acc[...] = jnp.zeros_like(acc)

    def turn(p):
        @pl.loop(0, hh)
        def _(h):
            for a in range(nb):
                x = qs[p, 16 * a:16 * (a + 1), h].astype(jnp.float32).reshape(16 * g, d)
                qt[h, a, p] = x.T.astype(jnp.bfloat16)

    q_in.wait()
    q_swap.wait_recv()
    for p in range(2):
        turn(p)

    def origin(slot):
        for h in range(hh):
            ox, oy = OFF[slot][h]
            src[slot + 1, h] = lax.rem(iy - oy + RING, RING) * RING + lax.rem(ix - ox + RING, RING)

    lane = lax.broadcasted_iota(jnp.int32, (16, w), 1)
    row = lax.broadcasted_iota(jnp.int32, (16, w), 0)
    lead = lax.rem(lane, w // 2) // g - row

    def attend(units, r0, r1, ahead=2):
        first = r0 // 16
        pieces = [(k, z) for k in units for z in range(2)]

        def scores(h, a):
            n = min(r1, 16 * (a + 1)) - r0
            q = jnp.concatenate([qt[h, a, 0], qt[h, a, 1]], axis=1)
            keys = jnp.concatenate([kv[k, h, 0, z, r0:r0 + n] for k, z in pieces], axis=0)
            sc[h, a, :len(pieces) * n] = jnp.dot(keys, q, preferred_element_type=jnp.float32)

        def weigh(h):
            vis = []
            for k, z in pieces:
                gap = 2 * (chip - src[k, h]) - z
                late = [jnp.where(gap + p >= 0, 0, 1) for p in range(2)]
                vis.append(lead >= jnp.where(lane < w // 2, late[0], late[1]))
            vt = jnp.concatenate([kv[k, h, 1, z, r0:r1] for k, z in pieces], axis=0).T
            for a in range(first, nb):
                n = min(r1, 16 * (a + 1)) - r0
                s = []
                for i in range(len(pieces)):
                    x = sc[h, a, i * n:(i + 1) * n]
                    if 16 * (a + 1) <= r1:
                        edge = jnp.where(vis[i], x[n - 16:], NEG)
                        x = jnp.concatenate([x[:n - 16], edge], axis=0) if n > 16 else edge
                    s.append(x)
                old = m_ref[h, a]
                new = jnp.maximum(old, jnp.max(functools.reduce(jnp.maximum, s), axis=0, keepdims=True))
                m_ref[h, a] = new
                fade = jnp.exp2((old - new) * c)
                top = new * c
                e = [jnp.exp2(x * c - top) for x in s]
                l_ref[h, a] = l_ref[h, a] * fade + jnp.sum(sum(e[1:], e[0]).reshape(n // 8, 8, w), axis=0)
                weights = []
                for x in e:
                    weights.append(x.astype(jnp.bfloat16))
                    if n < r1 - r0:
                        weights.append(jnp.zeros((r1 - r0 - n, w), jnp.bfloat16))
                pv = jnp.dot(vt, jnp.concatenate(weights, axis=0), preferred_element_type=jnp.float32)
                acc[h, a] = acc[h, a] * fade + pv

        for i in range(hh + ahead):
            if i < hh:
                for a in range(first, nb):
                    scores(i, a)
            if i >= ahead:
                weigh(i - ahead)

    def out(h, rows):
        return remote(ost.at[h, rows], o_ref.at[rows, hh * iz + h], out_sem.at[0], out_sem.at[1], {"cz": oz})

    def finish(a0, a1, together):
        @pl.loop(0, hh // together)
        def _(i):
            for h in [i * together + n for n in range(together)]:
                for a in range(a0, a1):
                    o = (acc[h, a] * (1.0 / jnp.sum(l_ref[h, a], axis=0, keepdims=True))).astype(jnp.bfloat16)
                    x = [o[:, p * 16 * g:(p + 1) * 16 * g].T.reshape(16, g, d) for p in range(2)]
                    here = iz == 0
                    ost[h, 16 * a:16 * (a + 1)] = jnp.where(here, x[1], x[0])
                    o_ref[16 * a:16 * (a + 1), hh * iz + h] = jnp.where(here, x[0], x[1])
            for h in [i * together + n for n in range(together)]:
                out(h, slice(16 * a0, 16 * a1)).start()

    def send_last(part):
        for slot in range(WHOLE, SLOTS):
            for n in range(4):
                unit(n, slot, part).start()

    def step(k, carry):
        for j in range(1, WHOLE + 1):
            @pl.when(k == j)
            def _():
                landed(kv.at[j], recv_sem.at[(j - 1) % RECVS])
                if j - 1 + AHEAD < WHOLE:
                    for n in range(4):
                        unit(n, j - 1 + AHEAD).start()
                if j - 1 + AHEAD == WHOLE:
                    send_last(0)
                if j - 1 + AHEAD == WHOLE + 1:
                    @pl.when(iz == 0)
                    def _():
                        send_last(1)
                if j == SLOTS - LAG:
                    @pl.when(iz == 1)
                    def _():
                        send_last(1)
        attend((k,), 0, t)
        return carry

    for h in range(hh):
        src[0, h] = chip
    for slot in range(SLOTS):
        origin(slot)
    swap.wait_send()
    q_swap.wait_send()
    lax.fori_loop(0, WHOLE + 1, step, 0)
    last = range(WHOLE + 1, SLOTS + 1)
    landed(kv.at[pl.ds(WHOLE + 1, 2), :, :, :, low], recv_sem.at[WHOLE % RECVS])
    attend(last, 0, t // 2)
    finish(0, nb // 2, 4)
    landed(kv.at[pl.ds(WHOLE + 1, 2), :, :, :, high], recv_sem.at[(WHOLE + 1) % RECVS])
    attend(last, t // 2, t, 2)
    finish(nb // 2, nb, 1)
    landed(kv.at[pl.ds(1, SLOTS)], send_sem.at[0])
    landed(ost, out_sem.at[0])
    landed(o_ref.at[:, pl.ds(hh * oz, hh)], out_sem.at[1])


def solution(mesh):
    assert mesh.shape["cx"] == RING and mesh.shape["cy"] == RING and mesh.shape["cz"] == 2
    spec = P(("dp", "cx", "cy", "cz"))

    def local(q, k, v):
        t, hq, d = q.shape
        hkv = k.shape[1]
        g = hq // hkv
        hh = hkv // 2
        nb = t // 16
        w = 2 * 16 * g
        units = SLOTS + 1
        o = pl.pallas_call(
            _kernel,
            out_shape=jax.ShapeDtypeStruct((t, hkv, g, d), jnp.bfloat16),
            in_specs=[pl.BlockSpec(memory_space=pltpu.HBM)] * 3,
            out_specs=pl.BlockSpec(memory_space=pltpu.VMEM),
            scratch_shapes=[
                pltpu.VMEM((t, hkv, d), jnp.bfloat16),
                pltpu.VMEM((t, hkv, d), jnp.bfloat16),
                pltpu.VMEM((hkv, 2, t, d), jnp.bfloat16),
                pltpu.VMEM((units, hh, 2, 2, t, d), jnp.bfloat16),
                pltpu.VMEM((2, t, hh, g, d), jnp.bfloat16),
                pltpu.VMEM((hh, nb, 2, d, 16 * g), jnp.bfloat16),
                pltpu.VMEM((hh, nb, d, w), jnp.float32),
                pltpu.VMEM((hh, nb, 1, w), jnp.float32),
                pltpu.VMEM((hh, nb, 8, w), jnp.float32),
                pltpu.VMEM((hh, t, g, d), jnp.bfloat16),
                pltpu.VMEM((hh, nb, 2 * t, w), jnp.float32),
                pltpu.SMEM((units, hh), jnp.int32),
                pltpu.SemaphoreType.DMA((3,)),
                pltpu.SemaphoreType.DMA((4,)),
                pltpu.SemaphoreType.DMA((1,)),
                pltpu.SemaphoreType.DMA((RECVS,)),
                pltpu.SemaphoreType.DMA((2,)),
            ],
            compiler_params=pltpu.CompilerParams(collective_id=0, has_side_effects=True, vmem_limit_bytes=20 << 20),
        )(*(pltpu.with_memory_space_constraint(x, pltpu.HBM) for x in (k, v, q.reshape(t, hkv, g, d))))
        return o.reshape(t, hq, d)

    return jax.shard_map(local, mesh=mesh, in_specs=(spec, spec, spec), out_specs=spec, check_vma=False)
```

```python
import functools
import math

import jax
import jax.numpy as jnp
from jax import lax
from jax.experimental import pallas as pl
from jax.experimental.pallas import tpu as pltpu
from jax.sharding import PartitionSpec as P

NEG = -1e30
RING = 4
LINKS = (("x", 1), ("x", -1), ("y", 1), ("y", -1))
HEAD_OF = {("x", 1): 0, ("x", -1): 1, ("y", 1): 2, ("y", -1): 3}
PLAN = (
    ("a", -1), ("b", -1), ("c", -1), ("d", -1), ("a", 0), ("c", 0), ("c", 1), ("d", 1),
    ("c", 4), ("c", 2), ("c", 5), ("c", 6), ("d", 0), ("c", 8), ("d", 4),
)
SLOTS = len(PLAN)
AHEAD = 4
RECVS = 2 * AHEAD
WHOLE = SLOTS - 2
LAG = 2


def _head(link, letter):
    axis, sign = link
    other = "y" if axis == "x" else "x"
    return HEAD_OF[{"a": (axis, sign), "b": (axis, -sign), "c": (other, sign), "d": (other, -sign)}[letter]]


def _offsets():
    off = [dict() for _ in range(SLOTS)]
    for slot, (letter, src) in enumerate(PLAN):
        for link in LINKS:
            head = _head(link, letter)
            x, y = (0, 0) if src < 0 else off[src][head]
            axis, sign = link
            x, y = (x + sign, y) if axis == "x" else (x, y + sign)
            assert head not in off[slot]
            off[slot][head] = (x % RING, y % RING)
    for head in range(len(LINKS)):
        assert len({off[s][head] for s in range(SLOTS)} | {(0, 0)}) == RING * RING
    return off


OFF = _offsets()


def _kernel(k_hbm, v_hbm, q_hbm, o_ref, kin, vin, st, kv, qs, qt, acc, m_ref, l_ref, ost, sc, src,
            in_sem, x_sem, send_sem, recv_sem, out_sem):
    t, hkv, d = k_hbm.shape
    g = q_hbm.shape[2]
    hh = hkv // 2
    nb = t // 16
    w = 2 * 16 * g
    iy, ix, iz = lax.axis_index("cx"), lax.axis_index("cy"), lax.axis_index("cz")
    oz = 1 - iz
    chip = iy * RING + ix
    c = d ** -0.5 * math.log2(math.e)

    def peer(link):
        axis, sign = link
        if axis == "x":
            return {"cy": lax.rem(ix + sign + RING, RING)}
        return {"cx": lax.rem(iy + sign + RING, RING)}

    low, high = slice(0, t // 2), slice(t // 2, t)

    k_in = pltpu.make_async_copy(k_hbm, kin, in_sem.at[0])
    v_in = pltpu.make_async_copy(v_hbm, vin, in_sem.at[1])
    q_in = pltpu.make_async_copy(q_hbm.at[:, pl.ds(hh * iz, hh)], qs.at[iz], in_sem.at[2])
    k_in.start()
    v_in.start()
    q_in.start()
    barrier = pltpu.get_barrier_semaphore()
    for link in LINKS:
        pl.semaphore_signal(barrier, inc=1, device_id=peer(link), device_id_type=pl.DeviceIdType.MESH)
    pl.semaphore_signal(barrier, inc=1, device_id={"cz": oz}, device_id_type=pl.DeviceIdType.MESH)

    for n, (ref, copy) in enumerate(((kin, k_in), (vin, v_in))):
        copy.wait()
        x = jnp.swapaxes(ref[...].astype(jnp.float32), 0, 1)
        st[:, n] = x.astype(jnp.bfloat16)

    def remote(a, b, s, r, to):
        return pltpu.make_async_remote_copy(
            src_ref=a, dst_ref=b, send_sem=s, recv_sem=r, device_id=to, device_id_type=pl.DeviceIdType.MESH)

    def unit(n, slot, part=0):
        link = LINKS[n]
        letter, arrival = PLAN[slot]
        h = _head(link, letter)
        here, there, to = kv.at[1 + arrival, h], kv.at[1 + slot, h], slot
        if slot < 2:
            z = (iz, oz)[part]
            here, there = (kv.at[0, h, :, z] if part else st.at[hh * iz + h]), there.at[:, z]
        elif slot >= WHOLE:
            rows, to = (low, high)[part], WHOLE + part
            here, there = here.at[:, :, rows], there.at[:, :, rows]
        return remote(here, there, send_sem.at[0], recv_sem.at[to % RECVS], peer(link))

    def landed(ref, sem):
        pltpu.make_async_copy(ref, ref, sem).wait()

    swap = remote(st.at[pl.ds(hh * oz, hh)], kv.at[0, :, :, iz], x_sem.at[0], x_sem.at[1], {"cz": oz})
    q_swap = remote(q_hbm.at[:, pl.ds(hh * oz, hh)], qs.at[iz], out_sem.at[0], in_sem.at[2], {"cz": oz})

    pl.semaphore_wait(barrier, len(LINKS) + 1)
    for n in range(4):
        unit(n, 0).start()
    swap.start()
    for n in range(4):
        unit(n, 1).start()
    for h in range(hh):
        kv[0, h, :, iz] = st[hh * iz + h]
    q_swap.start()
    swap.wait_recv()
    for slot in range(2):
        for n in range(4):
            unit(n, slot, 1).start()
    for slot in range(2, AHEAD):
        for n in range(4):
            unit(n, slot).start()

    m_ref[...] = jnp.full_like(m_ref, NEG)
    l_ref[...] = jnp.zeros_like(l_ref)
    acc[...] = jnp.zeros_like(acc)

    def turn(p):
        @pl.loop(0, hh)
        def _(h):
            for a in range(nb):
                x = qs[p, 16 * a:16 * (a + 1), h].astype(jnp.float32).reshape(16 * g, d)
                qt[h, a, p] = x.T.astype(jnp.bfloat16)

    landed(qs, in_sem.at[2])
    for p in range(2):
        turn(p)

    def origin(slot):
        for h in range(hh):
            ox, oy = OFF[slot][h]
            src[slot + 1, h] = lax.rem(iy - oy + RING, RING) * RING + lax.rem(ix - ox + RING, RING)

    lane = lax.broadcasted_iota(jnp.int32, (16, w), 1)
    row = lax.broadcasted_iota(jnp.int32, (16, w), 0)
    lead = lax.rem(lane, w // 2) // g - row

    def attend(units, r0, r1, ahead=2):
        first = r0 // 16
        pieces = [(k, z) for k in units for z in range(2)]

        def scores(h, a):
            n = min(r1, 16 * (a + 1)) - r0
            q = jnp.concatenate([qt[h, a, 0], qt[h, a, 1]], axis=1)
            keys = jnp.concatenate([kv[k, h, 0, z, r0:r0 + n] for k, z in pieces], axis=0)
            sc[h, a, :len(pieces) * n] = jnp.dot(keys, q, preferred_element_type=jnp.float32)

        def weigh(h):
            vis = []
            for k, z in pieces:
                gap = 2 * (chip - src[k, h]) - z
                late = [jnp.where(gap + p >= 0, 0, 1) for p in range(2)]
                vis.append(lead >= jnp.where(lane < w // 2, late[0], late[1]))
            vt = jnp.concatenate([kv[k, h, 1, z, r0:r1] for k, z in pieces], axis=0).T
            for a in range(first, nb):
                n = min(r1, 16 * (a + 1)) - r0
                s = []
                for i in range(len(pieces)):
                    x = sc[h, a, i * n:(i + 1) * n]
                    if 16 * (a + 1) <= r1:
                        edge = jnp.where(vis[i], x[n - 16:], NEG)
                        x = jnp.concatenate([x[:n - 16], edge], axis=0) if n > 16 else edge
                    s.append(x)
                old = m_ref[h, a]
                new = jnp.maximum(old, jnp.max(functools.reduce(jnp.maximum, s), axis=0, keepdims=True))
                m_ref[h, a] = new
                fade = jnp.exp2((old - new) * c)
                top = new * c
                e = [jnp.exp2(x * c - top) for x in s]
                l_ref[h, a] = l_ref[h, a] * fade + jnp.sum(sum(e[1:], e[0]).reshape(n // 8, 8, w), axis=0)
                weights = []
                for x in e:
                    weights.append(x.astype(jnp.bfloat16))
                    if n < r1 - r0:
                        weights.append(jnp.zeros((r1 - r0 - n, w), jnp.bfloat16))
                pv = jnp.dot(vt, jnp.concatenate(weights, axis=0), preferred_element_type=jnp.float32)
                acc[h, a] = acc[h, a] * fade + pv

        for i in range(hh + ahead):
            if i < hh:
                for a in range(first, nb):
                    scores(i, a)
            if i >= ahead:
                weigh(i - ahead)

    def out(h, rows):
        return remote(ost.at[h, rows], o_ref.at[rows, hh * iz + h], out_sem.at[0], out_sem.at[1], {"cz": oz})

    def finish(a0, a1, together):
        @pl.loop(0, hh // together)
        def _(i):
            for h in [i * together + n for n in range(together)]:
                for a in range(a0, a1):
                    o = (acc[h, a] * (1.0 / jnp.sum(l_ref[h, a], axis=0, keepdims=True))).astype(jnp.bfloat16)
                    x = [o[:, p * 16 * g:(p + 1) * 16 * g].T.reshape(16, g, d) for p in range(2)]
                    here = iz == 0
                    ost[h, 16 * a:16 * (a + 1)] = jnp.where(here, x[1], x[0])
                    o_ref[16 * a:16 * (a + 1), hh * iz + h] = jnp.where(here, x[0], x[1])
            for h in [i * together + n for n in range(together)]:
                out(h, slice(16 * a0, 16 * a1)).start()

    def send_last(part):
        for slot in range(WHOLE, SLOTS):
            for n in range(4):
                unit(n, slot, part).start()

    def step(k, carry):
        for j in range(1, WHOLE + 1):
            @pl.when(k == j)
            def _():
                landed(kv.at[j], recv_sem.at[(j - 1) % RECVS])
                if j - 1 + AHEAD < WHOLE:
                    for n in range(4):
                        unit(n, j - 1 + AHEAD).start()
                if j - 1 + AHEAD == WHOLE:
                    send_last(0)
                if j - 1 + AHEAD == WHOLE + 1:
                    @pl.when(iz == 0)
                    def _():
                        send_last(1)
                if j == SLOTS - LAG:
                    @pl.when(iz == 1)
                    def _():
                        send_last(1)
        attend((k,), 0, t)
        return carry

    for h in range(hh):
        src[0, h] = chip
    for slot in range(SLOTS):
        origin(slot)
    swap.wait_send()
    lax.fori_loop(0, WHOLE + 1, step, 0)
    last = range(WHOLE + 1, SLOTS + 1)
    landed(kv.at[pl.ds(WHOLE + 1, 2), :, :, :, low], recv_sem.at[WHOLE % RECVS])
    attend(last, 0, t // 2)
    finish(0, nb // 2, 4)
    landed(kv.at[pl.ds(WHOLE + 1, 2), :, :, :, high], recv_sem.at[(WHOLE + 1) % RECVS])
    attend(last, t // 2, t, 2)
    finish(nb // 2, nb, 1)
    landed(kv.at[pl.ds(1, SLOTS)], send_sem.at[0])
    landed(o_ref, out_sem.at[0])
    landed(o_ref.at[:, pl.ds(hh * oz, hh)], out_sem.at[1])


def solution(mesh):
    assert mesh.shape["cx"] == RING and mesh.shape["cy"] == RING and mesh.shape["cz"] == 2
    spec = P(("dp", "cx", "cy", "cz"))

    def local(q, k, v):
        t, hq, d = q.shape
        hkv = k.shape[1]
        g = hq // hkv
        hh = hkv // 2
        nb = t // 16
        w = 2 * 16 * g
        units = SLOTS + 1
        o = pl.pallas_call(
            _kernel,
            out_shape=jax.ShapeDtypeStruct((t, hkv, g, d), jnp.bfloat16),
            in_specs=[pl.BlockSpec(memory_space=pltpu.HBM)] * 3,
            out_specs=pl.BlockSpec(memory_space=pltpu.VMEM),
            scratch_shapes=[
                pltpu.VMEM((t, hkv, d), jnp.bfloat16),
                pltpu.VMEM((t, hkv, d), jnp.bfloat16),
                pltpu.VMEM((hkv, 2, t, d), jnp.bfloat16),
                pltpu.VMEM((units, hh, 2, 2, t, d), jnp.bfloat16),
                pltpu.VMEM((2, t, hh, g, d), jnp.bfloat16),
                pltpu.VMEM((hh, nb, 2, d, 16 * g), jnp.bfloat16),
                pltpu.VMEM((hh, nb, d, w), jnp.float32),
                pltpu.VMEM((hh, nb, 1, w), jnp.float32),
                pltpu.VMEM((hh, nb, 8, w), jnp.float32),
                pltpu.VMEM((hh, t, g, d), jnp.bfloat16),
                pltpu.VMEM((hh, nb, 2 * t, w), jnp.float32),
                pltpu.SMEM((units, hh), jnp.int32),
                pltpu.SemaphoreType.DMA((3,)),
                pltpu.SemaphoreType.DMA((2,)),
                pltpu.SemaphoreType.DMA((1,)),
                pltpu.SemaphoreType.DMA((RECVS,)),
                pltpu.SemaphoreType.DMA((2,)),
            ],
            compiler_params=pltpu.CompilerParams(collective_id=0, has_side_effects=True, vmem_limit_bytes=20 << 20),
        )(*(pltpu.with_memory_space_constraint(x, pltpu.HBM) for x in (k, v, q.reshape(t, hkv, g, d))))
        return o.reshape(t, hq, d)

    return jax.shard_map(local, mesh=mesh, in_specs=(spec, spec, spec), out_specs=spec, check_vma=False)
```
